256 devices in a mesh: grp: 8 (over y_hi, x), dev: 32 (over z, y_lo, core).
Axes of the slice: x: 4, y: 4 (y_hi: 2, y_lo: 2; y = y_hi * 2 + y_lo), z: 8, core: 2. Of those that a mesh axis runs over, the one named last changes fastest.
Arguments:
- queries: bfloat16 [32768, 256], P(('grp', 'dev')), may hold values from -32 to 32
- items: bfloat16 [32768, 256], P(('grp', 'dev')), may hold values from -24 to 24
- item_ids: int32 [32768], P('grp'), may hold values from 0 to 262143
- neg_embed: bfloat16 [16384, 256], P('dev'), may hold values from -6 to 6
- neg_logq: float32 [16384], P('dev'), may hold values from -12 to -8
- logq_table: float32 [262144], replicated, may hold values from -11 to -9.5
Outputs:
- query_loss: float32 [32768], P(('grp', 'dev'))
- query_grad: float32 [32768, 256], P(('grp', 'dev'))
- item_grad: float32 [32768, 256], P(('grp', 'dev'))
- negative_grad: float32 [16384, 256], P('dev')
The draws below stay inside these ranges and needn't reach their ends.
Inputs may be any that keep to these rules, and one draw needn't show every extreme that they name: `item_ids`: a row of logq_table.
All inputs are finite; a program needn't handle non-finite values.
Results may differ from the reference program's by a relative error of at most 0.0036.
Values may be sent and summed in bfloat16 or wider, within the bound.
A program may use at most 64 MiB of HBM per device.

```python
import math
import jax
import jax.numpy as jnp
import numpy as np
from jax import lax

D = 256
VOCAB = 262144
GROUP_ROWS = 4096
BATCH = 32768
NEG = 16384
N_GRP = 8


def joint_pair(key):
    base = jax.random.fold_in(key, 11)
    keys = jax.random.split(base, 8)
    queries = jax.random.normal(keys[0], (BATCH, D), jnp.float32)
    items = jax.random.normal(keys[1], (BATCH, D), jnp.float32)
    positions = jnp.arange(BATCH)
    leading = positions % 32 == 5
    trailing = positions % 32 == 6
    strength = jax.random.uniform(keys[4], (BATCH, 1), jnp.float32, 1.5, 2.5)
    target = jax.random.uniform(keys[7], (BATCH, 1), jnp.float32, 110.0, 320.0)
    squared = jnp.sum(items * items, axis=1, keepdims=True)
    lifted = items * jnp.sqrt(target / (0.25 * strength * squared))
    items = jnp.where(leading[:, None], lifted, items)
    spacing = jax.random.uniform(keys[5], (BATCH, 1), jnp.float32, 2.0, 2.5)
    lead_squared = jnp.sum(items * items, axis=1, keepdims=True)
    shrink = spacing / (0.25 * strength * lead_squared)
    follower = jnp.roll(items * (1.0 - shrink), 1, axis=0) + 0.005 * jax.random.normal(keys[6], (BATCH, D), jnp.float32)
    items = jnp.where(trailing[:, None], follower, items)
    queries = jnp.where(leading[:, None], strength * items, queries)
    return (jnp.clip(queries, -32.0, 32.0), jnp.clip(items, -24.0, 24.0))


def draw_queries(key, part):
    return joint_pair(key)[0].astype(jnp.bfloat16)


def draw_items(key, part):
    return joint_pair(key)[1].astype(jnp.bfloat16)


def touch_ends(entries, key, smallest, high):
    extent = entries.shape
    index_at = [jax.random.randint(jax.random.fold_in(key, axis), (), 0, extent[axis]) for axis in range(len(extent))]
    entries = entries.at[tuple(index_at)].set(smallest)
    longest = extent.index(max(extent))
    index_at[longest] = (index_at[longest] + 1) % extent[longest]
    return entries.at[tuple(index_at)].set(high)


def level_of(rng, extent, cuts, smallest, top_value):
    loudness, own = 1.0, jax.random.fold_in(rng, 6)
    for position, parts in cuts:
        steps = jnp.exp(jax.random.uniform(jax.random.fold_in(own, position), (parts,), jnp.float32, smallest / len(cuts), top_value / len(cuts)))
        loudness = loudness * jnp.repeat(steps, extent[position] // parts).reshape([-1 if axis == position else 1 for axis in range(len(extent))])
    return loudness


def ranked_wide(own_key, dims, count, lean):
    portions = [min(1 << octave, count + 1 - (1 << octave)) * (1 << 20) // math.isqrt((1 << octave) ** lean) + 1 for octave in range((count + 1).bit_length()) if 1 << octave <= count]
    scale = 1 + sum(portions) // (1 << 30)
    grid = np.cumsum(np.array([max(1, weight // scale) for weight in portions]))
    lot = jax.random.randint(jax.random.fold_in(own_key, 1), dims, 0, int(grid[len(portions) - 1]))
    start = jnp.left_shift(1, jnp.searchsorted(jnp.asarray(grid, jnp.int32), lot, side="right").astype(jnp.int32))
    grade = start - 1 + jax.random.randint(jax.random.fold_in(own_key, 4), dims, 0, 1 << 30) % jnp.minimum(start, count + 1 - start)
    return jax.random.permutation(jax.random.fold_in(own_key, 2), count)[grade].astype(jnp.int32)


def centred(own_key, extent, deviation, bound, pieces=(), kind=jnp.bfloat16):
    gain = level_of(own_key, extent, pieces, -0.22, 0.18) if pieces else 1.0
    result = jax.random.normal(own_key, extent, jnp.float32) * deviation * gain
    return jnp.minimum(jnp.maximum(result, -bound), bound).astype(kind)


def setup_inputs(seed: int = 0) -> dict:
    arg_keys = jax.random.split(jax.random.key(seed), 7)
    queries = draw_queries(jax.random.fold_in(arg_keys[6], 71), 0)
    items = draw_items(jax.random.fold_in(arg_keys[6], 71), 0)
    item_ids = touch_ends(ranked_wide(arg_keys[2], (BATCH,), VOCAB, 2), jax.random.fold_in(arg_keys[2], 3), 0, VOCAB - 1).astype(jnp.int32)
    neg_embed = centred(arg_keys[3], (NEG, D), 1.0, 6.0, ((0, 32),))
    neg_logq = jnp.clip(-12.0 + 4.0 * jax.random.uniform(arg_keys[4], (NEG,), jnp.float32) ** level_of(arg_keys[4], (NEG,), ((0, 32),), -0.2, 0.2), -12.0, -8.0)
    logq_table = jnp.clip(jax.random.uniform(arg_keys[5], (VOCAB,), jnp.float32, -11.0, -9.5), -11.0, -9.5)
    return {"queries": queries, "items": items, "item_ids": item_ids, "neg_embed": neg_embed, "neg_logq": neg_logq, "logq_table": logq_table}


logit_scale = 0.25


def reference(queries, items, item_ids, neg_embed, neg_logq, logq_table):
    item_offsets = jnp.take(logq_table, item_ids, axis=0)
    block_rows = min(512, GROUP_ROWS)
    block_count = GROUP_ROWS // block_rows
    grouped_q = queries.reshape(N_GRP, GROUP_ROWS, D)
    grouped_v = items.reshape(N_GRP, GROUP_ROWS, D)
    grouped_off = item_offsets.reshape(N_GRP, GROUP_ROWS)

    def one_group(packed):
        group_q, group_v, group_off = packed
        candidates = jnp.concatenate([group_v, neg_embed], axis=0)
        cand_offsets = jnp.concatenate([group_off, neg_logq], axis=0)
        columns = jnp.arange(GROUP_ROWS + NEG, dtype=jnp.int32)

        def one_block(summed, block_idx):
            first_row = block_idx * block_rows
            q_block = lax.dynamic_slice_in_dim(group_q, first_row, block_rows, 0)
            scores = logit_scale * jnp.dot(q_block, candidates.T, preferred_element_type=jnp.float32) - cand_offsets[None, :]
            row_max = jnp.max(scores, axis=1)
            log_norm = row_max + jnp.log(jnp.sum(jnp.exp(scores - row_max[:, None]), axis=1))
            targets = first_row + jnp.arange(block_rows, dtype=jnp.int32)
            positive_mask = columns[None, :] == targets[:, None]
            matched = jnp.sum(jnp.where(positive_mask, scores, 0.0), axis=1)
            logit_grad = (logit_scale * (jnp.exp(scores - log_norm[:, None]) - positive_mask.astype(jnp.float32))).astype(jnp.bfloat16)
            summed = summed + jnp.dot(logit_grad.T, q_block, preferred_element_type=jnp.float32)
            return summed, (log_norm - matched, jnp.dot(logit_grad, candidates, preferred_element_type=jnp.float32))

        zero_acc = jnp.zeros((GROUP_ROWS + NEG, D), jnp.float32)
        cand_grad, (losses, q_grads) = lax.scan(one_block, zero_acc, jnp.arange(block_count, dtype=jnp.int32))
        return losses.reshape(GROUP_ROWS), q_grads.reshape(GROUP_ROWS, D), cand_grad[:GROUP_ROWS], cand_grad[GROUP_ROWS:]

    losses, q_grads, v_grads, n_grads = lax.map(one_group, (grouped_q, grouped_v, grouped_off))
    return (losses.reshape(BATCH), q_grads.reshape(BATCH, D), v_grads.reshape(BATCH, D), jnp.sum(n_grads, axis=0))
```

```python
import functools

import jax
import jax.numpy as jnp
from jax import lax
from jax.experimental import pallas as pl
from jax.experimental.pallas import tpu as pltpu
from jax.sharding import PartitionSpec as P

MESH = pl.DeviceIdType.MESH
SCALE = 0.25
MASKED = -1e30
LANES = 128


def pair_order(nz):
    order = []
    for r in range(1, nz // 2):
        order += [r, nz - r]
    return order + [0, nz // 2]


def kernel(
    nz,
    nx,
    q_ref,
    v_ref,
    ids_ref,
    neg_ref,
    nlq_ref,
    tab_ref,
    loss_ref,
    qg_ref,
    vg_ref,
    ng_ref,
    q_all,
    cand,
    cand_t,
    offs,
    off_b,
    gat,
    scores,
    probs,
    probs2,
    cgrad,
    part,
    part_in,
    stat,
    stat_in,
    lz,
    lz_in,
    d2d_in,
    itm,
    itm_in,
    rs,
    rs_in,
    red,
    ag,
    q_sem,
    item_sem,
    neg_sem,
    off_sem,
    stat_sem,
    lz_sem,
    part_sem,
    d2d_sem,
    itm_sem,
    rs_sem,
    ag_sem,
):
    rows, width = q_ref.shape
    neg_rows = neg_ref.shape[0]
    shard = rows + neg_rows
    nyh = 2
    groups = nyh * nx
    cut = neg_rows // groups
    order = pair_order(nz)
    pos = {r: i for i, r in enumerate(order)}
    pairs = nz // 2

    g = lax.axis_index("grp")
    d = lax.axis_index("dev")
    yh, x = g // nx, g % nx
    z, yl, c = d // 4, (d // 2) % 2, d % 2

    def at(zz, dyl, dc):
        return zz * 4 + ((yl + dyl) % 2) * 2 + (c + dc) % 2

    def grp_at(dyh, dx):
        return ((yh + dyh) % 2) * nx + (x + dx) % nx

    def z_dev(r):
        return (g, at((z + r) % nz, 0, 0))

    plane = [
        (dyh, dx, dyl) for dyl in range(2) for dyh in range(nyh) for dx in range(nx)
    ]

    def mirror(dyh, dx, dyl):
        return plane.index((dyh, (nx - dx) % nx, dyl))

    started = []

    def push(src, dst, sems, i, device):
        copy = pltpu.make_async_remote_copy(
            src_ref=src,
            dst_ref=dst,
            send_sem=sems.at[0, i],
            recv_sem=sems.at[1, i],
            device_id=device,
            device_id_type=MESH,
        )
        copy.start()
        started.append(copy)
        return copy

    peers = [z_dev(r) for r in range(1, nz)]
    peers += [(g, at(z, j // 2, j % 2)) for j in (1, 2, 3)]
    peers += [(grp_at(1, 0), at(z, 1, 1))]
    peers += [
        (grp_at(dyh, dx), at(z, dyl, 0))
        for dyh, dx, dyl in plane
        if (dyh, dx) != (0, 0)
    ]
    barrier = pltpu.get_barrier_semaphore()
    for peer in peers:
        pl.semaphore_signal(barrier, inc=1, device_id=peer, device_id_type=MESH)

    def look(i, carry):
        entry = ids_ref[d * rows + i]
        row = tab_ref[pl.ds(lax.shift_right_logical(entry, 7), 1), :]
        lane = lax.broadcasted_iota(jnp.int32, (1, LANES), 1)
        gat[pl.ds(i, 1), :] = jnp.where(lane == (entry & 127), row, 0.0)
        return carry

    lax.fori_loop(0, rows, look, 0, unroll=8)
    offs[0, 0:1, :] = jnp.sum(gat[...].T, axis=0, keepdims=True)
    offs[0, 1 : 1 + neg_rows // LANES, :] = nlq_ref[...]

    pl.semaphore_wait(barrier, len(peers))

    q_copies, item_copies, neg_copies, off_copies = {}, {}, {}, {}
    for j in (1, 2, 3):
        device = (g, at(z, j // 2, j % 2))
        off_copies[j] = push(offs.at[0], offs.at[j], off_sem, j, device)
    for r in order:
        if r:
            q_copies[r] = push(
                q_ref, q_all.at[pl.ds(pos[r] * rows, rows)], q_sem, r, z_dev(nz - r)
            )
    for j in (1, 2, 3):
        device = (g, at(z, j // 2, j % 2))
        neg_device = (grp_at(1, 0), at(z, 1, 1)) if j == 3 else device
        item_copies[j] = push(
            v_ref, cand.at[pl.ds(j * shard, rows)], item_sem, j, device
        )
        neg_copies[j] = push(
            neg_ref, cand.at[pl.ds(j * shard + rows, neg_rows)], neg_sem, j, neg_device
        )

    q_all[pos[0] * rows : (pos[0] + 1) * rows, :] = q_ref[...]
    cand[0:rows, :] = v_ref[...]
    cand[rows:shard, :] = neg_ref[...]

    for j in range(4):
        if j:
            off_copies[j].wait_recv()
            item_copies[j].wait_recv()
            neg_copies[j].wait_recv()

        def turn(k, carry, j=j):
            line = jnp.broadcast_to(offs[j, pl.ds(k, 1), :], (LANES, LANES))
            off_b[pl.ds(j * shard + k * LANES, LANES), :] = line.T
            return carry

        lax.fori_loop(0, shard // LANES, turn, 0)
        for k in range(shard // LANES):
            lo = j * shard + k * LANES
            cand_t[:, lo : lo + LANES] = cand[lo : lo + LANES, :].T

    eye = lax.broadcasted_iota(jnp.int32, (rows, rows), 0) == lax.broadcasted_iota(
        jnp.int32, (rows, rows), 1
    )
    own_score = None
    tall = 4 * shard
    maxima = [None] * pairs

    def dot_nt(a, b):
        return lax.dot_general(
            a, b, (((1,), (1,)), ((), ())), preferred_element_type=jnp.float32
        )

    def fold(s, op):
        return op(s.reshape(s.shape[0] // 8, 8, s.shape[1]), axis=0)

    stat_copies = {}
    for p in range(pairs):
        for r in order[2 * p : 2 * p + 2]:
            if r:
                q_copies[r].wait_recv()
        scaled = q_all[2 * p * rows : (2 * p + 2) * rows, :] * jnp.bfloat16(SCALE)

        def slot_scores(j, scaled=scaled):
            s = dot_nt(cand[pl.ds(j * shard, shard), :], scaled)
            ob = off_b[pl.ds(j * shard, shard), :]
            return s - jnp.concatenate([ob, ob], axis=1)

        def forward(j, top, p=p, slot_scores=slot_scores):
            s = slot_scores(j)
            scores[p, pl.ds(j * shard, shard), :] = s
            return jnp.maximum(top, fold(s, jnp.max))

        if p == pairs - 1:
            s = slot_scores(0)
            corner = s[:rows, :rows]
            own_score = jnp.sum(jnp.where(eye, corner, 0.0), axis=0, keepdims=True)
            corner = jnp.where(eye, MASKED, corner)
            s = jnp.concatenate(
                [jnp.concatenate([corner, s[:rows, rows:]], axis=1), s[rows:]], axis=0
            )
            scores[p, 0:shard, :] = s
            top, first = fold(s, jnp.max), 1
        else:
            top, first = jnp.full((8, 2 * rows), MASKED, jnp.float32), 0
        top = lax.fori_loop(first, 4, forward, top)
        top = jnp.max(top, axis=0, keepdims=True)

        def weigh(t, total, p=p, top=top):
            e = jnp.exp(scores[p, pl.ds(t * LANES, LANES), :] - top)
            probs[pl.ds(t * LANES, LANES), :] = e.astype(jnp.bfloat16)
            return total + fold(e, jnp.sum)

        total = lax.fori_loop(
            0, tall // LANES, weigh, jnp.zeros((8, 2 * rows), jnp.float32)
        )
        total = jnp.sum(total, axis=0, keepdims=True)
        for h in range(2):
            r = order[2 * p + h]
            lanes = slice(h * rows, (h + 1) * rows)
            both = jnp.concatenate(
                [top[:, lanes], total[:, lanes], jnp.zeros((6, rows), jnp.float32)], axis=0
            )
            if r:
                stat[2 * p + h] = both
                back = nz - r
                stat_copies[back] = push(
                    stat.at[2 * p + h], stat_in.at[back], stat_sem, back, z_dev(r)
                )
            else:
                stat_in[0] = both
        qp = jnp.dot(cand_t[...], probs[...], preferred_element_type=jnp.float32)
        for h in range(2):
            part[2 * p + h] = qp[:, h * rows : (h + 1) * rows].astype(jnp.bfloat16)

    for r in range(1, nz):
        stat_copies[r].wait_recv()
    best = own_score
    for r in range(nz):
        best = jnp.maximum(best, stat_in[r, 0:1, :])
    mass = jnp.exp(own_score - best)
    for r in range(nz):
        mass = mass + stat_in[r, 1:2, :] * jnp.exp(stat_in[r, 0:1, :] - best)
    log_norm = best + jnp.log(mass)
    lz[...] = jnp.broadcast_to(log_norm, (8, rows))
    lz_copies = {}
    for r in order:
        if r:
            lz_copies[r] = push(lz, lz_in.at[pos[r]], lz_sem, r, z_dev(nz - r))
    lz_in[pos[0]] = jnp.broadcast_to(log_norm, (8, rows))
    loss_ref[...] = log_norm - own_score
    own_term = jnp.exp(own_score - log_norm) - 1.0

    part_copies = {}
    for r in order:
        if r:
            back = nz - r
            part_copies[back] = push(
                part.at[pos[r]], part_in.at[back], part_sem, back, z_dev(r)
            )

    for r in order:
        if r:
            lz_copies[r].wait_recv()

    d2d_copies = []
    core_mate = (g, at(z, 0, 1))
    for j in (1, 3, 0, 2):

        def again(t, carry, j=j):
            lo = j * shard + t * 64
            for p in range(pairs):
                norm = jnp.concatenate(
                    [lz_in[2 * p, 0:1, :], lz_in[2 * p + 1, 0:1, :]], axis=1
                )
                e = jnp.exp(scores[p, pl.ds(lo, 64), :] - norm)
                probs2[pl.ds(t * 64, 64), 2 * p * rows : (2 * p + 2) * rows] = e.astype(
                    jnp.bfloat16
                )
            return carry

        lax.fori_loop(0, shard // 64, again, 0)
        cgrad[j] = SCALE * jnp.dot(
            probs2[...], q_all[...], preferred_element_type=jnp.float32
        )
        if j in (1, 3):
            i = j // 2
            d2d_copies.append(push(cgrad.at[j], d2d_in.at[i], d2d_sem, i, core_mate))

    for i in range(2):
        d2d_copies[i].wait_recv()
    itm[...] = (cgrad[2, 0:rows, :] + d2d_in[1, 0:rows, :]).astype(jnp.bfloat16)
    rs_copies = {}
    for dyl in (1, 0):
        j = 2 * dyl
        rs[dyl] = (cgrad[j, rows:shard, :] + d2d_in[dyl, rows:shard, :]).astype(jnp.bfloat16)
        for dyh, dx, dy in plane:
            if dy == dyl and (dyh, dx, dy) != (0, 0, 0):
                target = grp_at(dyh, dx)
                i = mirror(dyh, dx, dy)
                rs_copies[i] = push(
                    rs.at[dyl, pl.ds(pl.multiple_of(target * cut, cut), cut)],
                    rs_in.at[i],
                    rs_sem,
                    i,
                    (target, at(z, dyl, 0)),
                )
    itm_copy = push(itm, itm_in, itm_sem, 0, (g, at(z, 1, 0)))

    own_rows = pl.ds(pl.multiple_of(g * cut, cut), cut)
    own_neg = pl.ds(pl.multiple_of(rows + g * cut, cut), cut)
    summed = cgrad[0, own_neg, :] + d2d_in[0, own_neg, :]
    for i in range(1, len(plane)):
        rs_copies[i].wait_recv()
        summed = summed + rs_in[i].astype(jnp.float32)
    red[...] = summed.astype(jnp.bfloat16)
    ag_copies = {}
    for dyh, dx, dyl in plane:
        if dyl == 0 and (dyh, dx) != (0, 0):
            i = mirror(dyh, dx, 0)
            ag_copies[i] = push(
                red, ag.at[own_rows], ag_sem, i, (grp_at(dyh, dx), at(z, 0, 0))
            )
    ag[own_rows, :] = summed.astype(jnp.bfloat16)

    acc = own_term * cand_t[:, 0:rows].astype(jnp.float32)
    for r in range(nz):
        if r:
            part_copies[r].wait_recv()
            piece = part_in[r]
        else:
            piece = part[pos[0]]
        share = jnp.exp(stat_in[r, 0:1, :] - log_norm)
        acc = acc + share * piece.astype(jnp.float32)
    qg_ref[...] = (SCALE * acc).T

    itm_copy.wait_recv()
    column = jnp.broadcast_to(own_term, (rows, rows)).T
    column = jnp.concatenate([column] * (width // rows), axis=1)
    vg_ref[...] = (
        cgrad[0, 0:rows, :]
        + d2d_in[0, 0:rows, :]
        + itm_in[...].astype(jnp.float32)
        + SCALE * column * q_ref[...].astype(jnp.float32)
    )

    for i in ag_copies:
        ag_copies[i].wait_recv()
    ng_ref[...] = ag[...].astype(jnp.float32)
    for copy in started:
        copy.wait_send()


def local(queries, items, item_ids, neg_embed, neg_logq, logq_table, *, nz, nx):
    rows, width = queries.shape
    neg_rows = neg_embed.shape[0]
    shard = rows + neg_rows
    tall = 4 * shard
    groups = 2 * nx
    cut = neg_rows // groups
    f32, bf16 = jnp.float32, jnp.bfloat16
    dma = pltpu.SemaphoreType.DMA
    vmem = pl.BlockSpec(memory_space=pltpu.VMEM)
    smem = pl.BlockSpec(memory_space=pltpu.SMEM)
    loss, qg, vg, ng = pl.pallas_call(
        functools.partial(kernel, nz, nx),
        out_shape=(
            jax.ShapeDtypeStruct((1, rows), f32),
            jax.ShapeDtypeStruct((rows, width), f32),
            jax.ShapeDtypeStruct((rows, width), f32),
            jax.ShapeDtypeStruct((neg_rows, width), f32),
        ),
        in_specs=[vmem, vmem, smem, vmem, vmem, vmem],
        out_specs=(vmem, vmem, vmem, vmem),
        scratch_shapes=[
            pltpu.VMEM((nz * rows, width), bf16),
            pltpu.VMEM((tall, width), bf16),
            pltpu.VMEM((width, tall), bf16),
            pltpu.VMEM((4, 8, LANES), f32),
            pltpu.VMEM((tall, LANES), f32),
            pltpu.VMEM((rows, LANES), f32),
            pltpu.VMEM((nz // 2, tall, 2 * rows), f32),
            pltpu.VMEM((tall, 2 * rows), bf16),
            pltpu.VMEM((shard, nz * rows), bf16),
            pltpu.VMEM((4, shard, width), f32),
            pltpu.VMEM((nz, width, rows), bf16),
            pltpu.VMEM((nz, width, rows), bf16),
            pltpu.VMEM((nz, 8, rows), f32),
            pltpu.VMEM((nz, 8, rows), f32),
            pltpu.VMEM((8, rows), f32),
            pltpu.VMEM((nz, 8, rows), f32),
            pltpu.VMEM((2, shard, width), f32),
            pltpu.VMEM((rows, width), bf16),
            pltpu.VMEM((rows, width), bf16),
            pltpu.VMEM((2, neg_rows, width), bf16),
            pltpu.VMEM((2 * groups, cut, width), bf16),
            pltpu.VMEM((cut, width), bf16),
            pltpu.VMEM((neg_rows, width), bf16),
            dma((2, nz)),
            dma((2, 4)),
            dma((2, 4)),
            dma((2, 4)),
            dma((2, nz)),
            dma((2, nz)),
            dma((2, nz)),
            dma((2, 2)),
            dma((2, 1)),
            dma((2, 2 * groups)),
            dma((2, 2 * groups)),
        ],
        compiler_params=pltpu.CompilerParams(
            collective_id=0, has_side_effects=True, vmem_limit_bytes=60 << 20
        ),
    )(
        queries,
        items,
        item_ids,
        neg_embed,
        neg_logq.reshape(-1, LANES),
        logq_table.reshape(-1, LANES),
    )
    return loss.reshape(rows), qg, vg, ng


def solution(mesh):
    return jax.shard_map(
        functools.partial(
            local, nz=mesh.shape["dev"] // 4, nx=mesh.shape["grp"] // 2
        ),
        mesh=mesh,
        in_specs=(
            P(("grp", "dev"), None),
            P(("grp", "dev"), None),
            P("grp"),
            P("dev", None),
            P("dev"),
            P(),
        ),
        out_specs=(
            P(("grp", "dev")),
            P(("grp", "dev"), None),
            P(("grp", "dev"), None),
            P("dev", None),
        ),
        check_vma=False,
    )
```

```python
import functools

import jax
import jax.numpy as jnp
from jax import lax
from jax.experimental import pallas as pl
from jax.experimental.pallas import tpu as pltpu
from jax.sharding import PartitionSpec as P

MESH = pl.DeviceIdType.MESH
SCALE = 0.25
MASKED = -1e30
LANES = 128
DIRECT = 192


def pair_order(nz):
    order = [0, 1]
    for r in range(1, nz // 2):
        order += [nz - r, r + 1]
    return order


def dot_nt(a, b):
    return lax.dot_general(
        a, b, (((1,), (1,)), ((), ())), preferred_element_type=jnp.float32
    )


def fold(s, op):
    return op(s.reshape(s.shape[0] // 8, 8, s.shape[1]), axis=0)


def kernel(
    nz,
    nx,
    q_hbm,
    v_hbm,
    ids_hbm,
    neg_hbm,
    nlq_hbm,
    tab_hbm,
    loss_ref,
    qg_ref,
    vg_ref,
    ag,
    ids_ref,
    tab_ref,
    nlq_ref,
    q_all,
    cand,
    cand_t,
    offs,
    off_b,
    gat,
    scores,
    probs,
    probs2,
    cgrad,
    part,
    part_in,
    stat,
    stat_in,
    lz,
    lz_in,
    d2d,
    d2d_in,
    itm,
    itm_in,
    rs,
    rs_in,
    red,
    in_sem,
    q_sem,
    cand_sem,
    off_sem,
    stat_sem,
    lz_sem,
    part_sem,
    d2d_sem,
    itm_sem,
    rs_sem,
    ag_sem,
):
    rows, width = qg_ref.shape
    neg_rows = ag.shape[0]
    shard = rows + neg_rows
    tall = 4 * shard
    nyh = 2
    groups = nyh * nx
    cut = neg_rows // groups
    order = pair_order(nz)
    pos = {r: i for i, r in enumerate(order)}
    pairs = nz // 2
    early = max(1, pairs // 2)
    ahead = max(0, pairs - 2)

    g = lax.axis_index("grp")
    d = lax.axis_index("dev")
    yh, x = g // nx, g % nx
    z, yl, c = d // 4, (d // 2) % 2, d % 2

    def at(zz, dyl, dc):
        return zz * 4 + ((yl + dyl) % 2) * 2 + (c + dc) % 2

    def grp_at(dyh, dx):
        return ((yh + dyh) % 2) * nx + (x + dx) % nx

    def z_dev(r):
        return (g, at((z + r) % nz, 0, r))

    def distance(dyh, dx, dyl):
        return min(dx, nx - dx) + (1 if dyl else 2 * dyh)

    plane = [
        (dyh, dx, dyl) for dyl in range(2) for dyh in range(nyh) for dx in range(nx)
    ]
    far_first = sorted(plane, key=lambda t: -distance(*t))

    def mirror(dyh, dx, dyl):
        return plane.index((dyh, (nx - dx) % nx, dyl))

    started = []

    def push(src, dst, sems, i, device):
        copy = pltpu.make_async_remote_copy(
            src_ref=src,
            dst_ref=dst,
            send_sem=sems.at[0, i],
            recv_sem=sems.at[1, i],
            device_id=device,
            device_id_type=MESH,
        )
        copy.start()
        started.append(copy)
        return copy

    def rows_of(start, size):
        return pl.ds(start, size)

    loads = [
        pltpu.make_async_copy(q_hbm, q_all.at[rows_of(0, rows)], in_sem.at[0]),
        pltpu.make_async_copy(v_hbm, cand.at[rows_of(0, rows)], in_sem.at[1]),
        pltpu.make_async_copy(neg_hbm, cand.at[rows_of(rows, neg_rows)], in_sem.at[2]),
        pltpu.make_async_copy(ids_hbm, ids_ref, in_sem.at[3]),
        pltpu.make_async_copy(tab_hbm, tab_ref, in_sem.at[4]),
        pltpu.make_async_copy(nlq_hbm, nlq_ref, in_sem.at[5]),
    ]
    for load in loads:
        load.start()

    core_mate = (g, at(z, 0, 1))
    y_mate = (g, at(z, 1, 0))
    y_wrap = (grp_at(1, 0), at(z, 1, 0))
    peers = [z_dev(r) for r in range(1, nz)]
    peers += [(g, at(z, j // 2, j % 2)) for j in (1, 2, 3)]
    peers += [y_wrap]
    peers += [
        (grp_at(dyh, dx), at(z, dyl, 1))
        for dyh, dx, dyl in plane
        if (dyh, dx) != (0, 0)
    ]
    barrier = pltpu.get_barrier_semaphore()
    for peer in peers:
        pl.semaphore_signal(barrier, inc=1, device_id=peer, device_id_type=MESH)
    for load in loads[:3]:
        load.wait()
    pl.semaphore_wait(barrier, len(peers))

    q_copies = {}
    mid = nz // 2

    def hop(k):
        for side in range(2):
            held, new = ((nz - k) % nz, nz - k - 1) if side else (k, k + 1)
            first, size, i = 0, rows, new
            if new == mid:
                first, size, i = side * rows // 2, rows // 2, mid + side * (nz - mid)
            q_copies[i] = push(
                q_all.at[rows_of(pos[held] * rows + first, size)],
                q_all.at[rows_of(pos[new] * rows + first, size)],
                q_sem,
                i,
                z_dev(1 if side else nz - 1),
            )

    reached = set()

    def reach(k):
        if k in reached:
            return
        reached.add(k)
        for i in (k, nz if k == mid else nz - k):
            q_copies[i].wait_recv()
        if k < mid:
            hop(k)

    hop(0)

    def shift(lo, size, j, i, device):
        return push(
            cand.at[rows_of(lo, size)],
            cand.at[rows_of(j * shard + lo, size)],
            cand_sem,
            i,
            device,
        )

    cut_at = rows + DIRECT
    y_copies = [
        shift(0, cut_at, 2, 0, y_mate),
        shift(cut_at, shard - cut_at, 2, 1, y_wrap),
    ]
    mate_copy = shift(0, shard, 1, 2, core_mate)

    for load in loads[3:]:
        load.wait()

    def look(i, carry):
        entry = ids_ref[d * rows + i]
        row = tab_ref[pl.ds(lax.shift_right_logical(entry, 7), 1), :]
        lane = lax.broadcasted_iota(jnp.int32, (1, LANES), 1)
        gat[pl.ds(i, 1), :] = jnp.where(lane == (entry & 127), row, 0.0)
        return carry

    lax.fori_loop(0, rows, look, 0, unroll=8)
    offs[0, 0:1, :] = jnp.sum(gat[...].T, axis=0, keepdims=True)
    offs[0, 1 : 1 + neg_rows // LANES, :] = nlq_ref[...]
    off_copies = {}
    for j in (1, 2, 3):
        off_copies[j] = push(
            offs.at[0], offs.at[j], off_sem, j, (g, at(z, j // 2, j % 2))
        )

    eye = lax.broadcasted_iota(jnp.int32, (rows, rows), 0) == lax.broadcasted_iota(
        jnp.int32, (rows, rows), 1
    )
    own = {}

    def prepare(j):
        for k in range(shard // LANES):
            lo = j * shard + k * LANES
            cand_t[:, lo : lo + LANES] = cand[lo : lo + LANES, :].T
        if j:
            off_copies[j].wait_recv()
        for k in range(shard // LANES):
            lo = j * shard + k * LANES
            line = jnp.broadcast_to(offs[j, k : k + 1, :], (LANES, LANES))
            off_b[lo : lo + LANES, :] = line.T

    def score(p, lo, size):
        scaled = q_all[2 * p * rows : (2 * p + 2) * rows, :] * jnp.bfloat16(SCALE)
        ob = off_b[lo : lo + size, :]
        s = dot_nt(cand[lo : lo + size, :], scaled) - jnp.concatenate([ob, ob], axis=1)
        if p == 0 and lo == 0:
            corner = s[:rows, :rows]
            own["score"] = jnp.sum(jnp.where(eye, corner, 0.0), axis=0, keepdims=True)
            corner = jnp.where(eye, MASKED, corner)
            s = jnp.concatenate(
                [jnp.concatenate([corner, s[:rows, rows:]], axis=1), s[rows:]], axis=0
            )
        scores[p, lo : lo + size, :] = s
        return jnp.max(fold(s, jnp.max), axis=0, keepdims=True)

    def weigh(p, lo, size, top):
        total = jnp.zeros((8, 2 * rows), jnp.float32)
        for at_row in range(lo, lo + size, LANES):
            e = jnp.exp(scores[p, at_row : at_row + LANES, :] - top)
            probs[p, at_row : at_row + LANES, :] = e.astype(jnp.bfloat16)
            total = total + fold(e, jnp.sum)
        return jnp.sum(total, axis=0, keepdims=True)

    def pull(p, lo, size):
        return jnp.dot(
            cand_t[:, lo : lo + size],
            probs[p, lo : lo + size, :],
            preferred_element_type=jnp.float32,
        )

    stat_copies = {}

    def tell(p, top, total):
        for h in range(2):
            r = order[2 * p + h]
            lanes = slice(h * rows, (h + 1) * rows)
            both = jnp.concatenate(
                [top[:, lanes], total[:, lanes], jnp.zeros((6, rows), jnp.float32)], axis=0
            )
            if r:
                stat[2 * p + h] = both
                back = nz - r
                stat_copies[back] = push(
                    stat.at[2 * p + h], stat_in.at[back], stat_sem, back, z_dev(r)
                )
            else:
                stat_in[0] = both

    def keep(p, qp):
        for h in range(2):
            part[2 * p + h] = qp[:, h * rows : (h + 1) * rows].astype(jnp.bfloat16)

    half = 2 * shard
    prepare(0)
    mate_copy.wait_recv()
    prepare(1)
    tops, totals, ratios = [], [], []
    for p in range(early):
        reach(p + 1)
        tops.append(score(p, 0, half))
        totals.append(weigh(p, 0, half, tops[p]))
        if p == 0:
            for copy in y_copies:
                copy.wait_recv()
            relay = push(
                cand.at[rows_of(2 * shard, shard)],
                cand.at[rows_of(3 * shard, shard)],
                cand_sem,
                3,
                core_mate,
            )
    prepare(2)
    relay.wait_recv()
    prepare(3)
    for p in range(early):
        top = jnp.maximum(tops[p], score(p, half, half))
        total = weigh(p, half, half, top)
        ratios.append(jnp.exp(tops[p] - top))
        tell(p, top, ratios[p] * totals[p] + total)
        if p == 0 and early < pairs:
            reach(early + 1)
    for p in range(early, pairs):
        reach(p + 1)
        top = score(p, 0, tall)
        total = weigh(p, 0, tall, top)
        tell(p, top, total)
    for p in reversed(range(pairs)):
        if p < early:
            keep(p, ratios[p] * pull(p, 0, half) + pull(p, half, half))
        else:
            keep(p, pull(p, 0, tall))

    for r in range(1, nz):
        stat_copies[r].wait_recv()
    own_score = own["score"]
    best = own_score
    for r in range(nz):
        best = jnp.maximum(best, stat_in[r, 0:1, :])
    mass = jnp.exp(own_score - best)
    for r in range(nz):
        mass = mass + stat_in[r, 1:2, :] * jnp.exp(stat_in[r, 0:1, :] - best)
    log_norm = best + jnp.log(mass)
    lz[...] = jnp.broadcast_to(log_norm, (8, rows))
    lz_copies = {}
    for r in reversed(order):
        if r:
            lz_copies[r] = push(lz, lz_in.at[pos[r]], lz_sem, r, z_dev(nz - r))
    lz_in[pos[0]] = jnp.broadcast_to(log_norm, (8, rows))
    part_copies = {}
    for r in reversed(order):
        if r:
            back = nz - r
            part_copies[back] = push(
                part.at[pos[r]], part_in.at[back], part_sem, back, z_dev(r)
            )
    loss_ref[...] = log_norm - own_score
    own_term = jnp.exp(own_score - log_norm) - 1.0

    def await_lz(p):
        for r in order[2 * p : 2 * p + 2]:
            if r:
                lz_copies[r].wait_recv()

    def again(p, lo, size, lane):
        norm = jnp.concatenate([lz_in[2 * p, 0:1, :], lz_in[2 * p + 1, 0:1, :]], axis=1)

        for at_row in range(lo, lo + size, LANES):
            e = jnp.exp(scores[p, at_row : at_row + LANES, :] - norm)
            probs2[at_row : at_row + LANES, 2 * lane * rows : (2 * lane + 2) * rows] = (
                e.astype(jnp.bfloat16)
            )

    def gather_grad(lo, size, first, last):
        return jnp.dot(
            probs2[lo : lo + size, 0 : 2 * (last - first) * rows],
            q_all[2 * first * rows : 2 * last * rows, :],
            preferred_element_type=jnp.float32,
        )

    if ahead:
        for p in range(ahead):
            await_lz(p)
            again(p, 0, tall, p)
        for j in range(4):
            cgrad[j] = gather_grad(j * shard, shard, 0, ahead)
    for p in range(ahead, pairs):
        await_lz(p)
    d2d_copies = {}
    for j in (3, 1, 2, 0):
        for p in range(ahead, pairs):
            again(p, j * shard, shard, p - ahead)
        grad = gather_grad(j * shard, shard, ahead, pairs)
        if ahead:
            grad = grad + cgrad[j]
        grad = SCALE * grad
        if j in (3, 1):
            i = j // 2
            d2d[i] = grad.astype(jnp.bfloat16)
            d2d_copies[i] = push(d2d.at[i], d2d_in.at[i], d2d_sem, i, core_mate)
        else:
            cgrad[j] = grad

    rs_copies = {}
    for dyl in (1, 0):
        d2d_copies[dyl].wait_recv()
        whole = cgrad[2 * dyl] + d2d_in[dyl].astype(jnp.float32)
        rs[dyl] = whole[rows:].astype(jnp.bfloat16)
        for dyh, dx, dy in far_first:
            if dy == dyl:
                target = grp_at(dyh, dx)
                i = mirror(dyh, dx, dy)
                rs_copies[i] = push(
                    rs.at[dyl, rows_of(pl.multiple_of(target * cut, cut), cut)],
                    rs_in.at[i],
                    rs_sem,
                    i,
                    (target, at(z, dyl, 1)),
                )
        if dyl:
            itm[...] = whole[:rows].astype(jnp.bfloat16)
            itm_copy = push(itm, itm_in, itm_sem, 0, y_mate)
        else:
            cgrad[0] = whole

    own_rows = rows_of(pl.multiple_of(g * cut, cut), cut)
    summed = jnp.zeros((cut, width), jnp.float32)
    for i in range(len(plane)):
        rs_copies[i].wait_recv()
        summed = summed + rs_in[i].astype(jnp.float32)
    red[...] = summed.astype(jnp.bfloat16)
    ag_copies = {}
    for dyh, dx, dyl in far_first:
        if dyl == 0:
            i = mirror(dyh, dx, 0)
            ag_copies[i] = push(
                red, ag.at[own_rows], ag_sem, i, (grp_at(dyh, dx), at(z, 0, 1))
            )

    acc = own_term * cand_t[:, 0:rows].astype(jnp.float32)
    for r in range(nz):
        if r:
            part_copies[r].wait_recv()
            piece = part_in[r]
        else:
            piece = part[pos[0]]
        share = jnp.exp(stat_in[r, 0:1, :] - log_norm)
        acc = acc + share * piece.astype(jnp.float32)
    qg_ref[...] = (SCALE * acc).T

    itm_copy.wait_recv()
    column = jnp.broadcast_to(own_term, (rows, rows)).T
    column = jnp.concatenate([column] * (width // rows), axis=1)
    vg_ref[...] = (
        cgrad[0, 0:rows, :]
        + itm_in[...].astype(jnp.float32)
        + SCALE * column * q_all[0:rows, :].astype(jnp.float32)
    )

    for i in ag_copies:
        ag_copies[i].wait_recv()
    for copy in started:
        copy.wait_send()


def emit(loss_in, qg_in, vg_in, ng_in, loss_ref, qg_ref, vg_ref, ng_ref):
    loss_ref[...] = loss_in[...]
    qg_ref[...] = qg_in[...]
    vg_ref[...] = vg_in[...]
    ng_ref[...] = ng_in[...].astype(jnp.float32)


def local(queries, items, item_ids, neg_embed, neg_logq, logq_table, *, nz, nx):
    rows, width = queries.shape
    neg_rows = neg_embed.shape[0]
    shard = rows + neg_rows
    tall = 4 * shard
    groups = 2 * nx
    cut = neg_rows // groups
    pairs = nz // 2
    f32, bf16 = jnp.float32, jnp.bfloat16
    dma = pltpu.SemaphoreType.DMA
    vmem = pl.BlockSpec(memory_space=pltpu.VMEM)
    away = pl.BlockSpec(memory_space=pl.ANY)
    table = logq_table.reshape(-1, LANES)
    neg_lines = neg_logq.reshape(-1, LANES)
    results = pl.pallas_call(
        functools.partial(kernel, nz, nx),
        out_shape=(
            jax.ShapeDtypeStruct((1, rows), f32),
            jax.ShapeDtypeStruct((rows, width), f32),
            jax.ShapeDtypeStruct((rows, width), f32),
            jax.ShapeDtypeStruct((neg_rows, width), bf16),
        ),
        in_specs=[away] * 6,
        out_specs=(vmem, vmem, vmem, vmem),
        scratch_shapes=[
            pltpu.SMEM(item_ids.shape, jnp.int32),
            pltpu.VMEM(table.shape, f32),
            pltpu.VMEM(neg_lines.shape, f32),
            pltpu.VMEM((nz * rows, width), bf16),
            pltpu.VMEM((tall, width), bf16),
            pltpu.VMEM((width, tall), bf16),
            pltpu.VMEM((4, 8, LANES), f32),
            pltpu.VMEM((tall, LANES), f32),
            pltpu.VMEM((rows, LANES), f32),
            pltpu.VMEM((pairs, tall, 2 * rows), f32),
            pltpu.VMEM((pairs, tall, 2 * rows), bf16),
            pltpu.VMEM((tall, 4 * rows), bf16),
            pltpu.VMEM((4, shard, width), f32),
            pltpu.VMEM((nz, width, rows), bf16),
            pltpu.VMEM((nz, width, rows), bf16),
            pltpu.VMEM((nz, 8, rows), f32),
            pltpu.VMEM((nz, 8, rows), f32),
            pltpu.VMEM((8, rows), f32),
            pltpu.VMEM((nz, 8, rows), f32),
            pltpu.VMEM((2, shard, width), bf16),
            pltpu.VMEM((2, shard, width), bf16),
            pltpu.VMEM((rows, width), bf16),
            pltpu.VMEM((rows, width), bf16),
            pltpu.VMEM((2, neg_rows, width), bf16),
            pltpu.VMEM((2 * groups, cut, width), bf16),
            pltpu.VMEM((cut, width), bf16),
            dma((6,)),
            dma((2, nz + 1)),
            dma((2, 4)),
            dma((2, 4)),
            dma((2, nz)),
            dma((2, nz)),
            dma((2, nz)),
            dma((2, 2)),
            dma((2, 1)),
            dma((2, 2 * groups)),
            dma((2, 2 * groups)),
        ],
        compiler_params=pltpu.CompilerParams(
            collective_id=0, has_side_effects=True, vmem_limit_bytes=60 << 20
        ),
    )(queries, items, item_ids, neg_embed, neg_lines, table)
    loss, qg, vg, ng = pl.pallas_call(
        emit,
        out_shape=(
            jax.ShapeDtypeStruct((1, rows), f32),
            jax.ShapeDtypeStruct((rows, width), f32),
            jax.ShapeDtypeStruct((rows, width), f32),
            jax.ShapeDtypeStruct((neg_rows, width), f32),
        ),
        in_specs=[vmem] * 4,
        out_specs=(vmem, vmem, vmem, vmem),
    )(*results)
    return loss.reshape(rows), qg, vg, ng


def solution(mesh):
    return jax.shard_map(
        functools.partial(
            local, nz=mesh.shape["dev"] // 4, nx=mesh.shape["grp"] // 2
        ),
        mesh=mesh,
        in_specs=(
            P(("grp", "dev"), None),
            P(("grp", "dev"), None),
            P("grp"),
            P("dev", None),
            P("dev"),
            P(),
        ),
        out_specs=(
            P(("grp", "dev")),
            P(("grp", "dev"), None),
            P(("grp", "dev"), None),
            P("dev", None),
        ),
        check_vma=False,
    )
```

```python
import functools

import jax
import jax.numpy as jnp
from jax import lax
from jax.experimental import pallas as pl
from jax.experimental.pallas import tpu as pltpu
from jax.sharding import PartitionSpec as P

MESH = pl.DeviceIdType.MESH
SCALE = 0.25
MASKED = -1e30
LANES = 128
DIRECT = 192


def pair_order(nz):
    order = [0, 1]
    for r in range(1, nz // 2):
        order += [nz - r, r + 1]
    return order


def dot_nt(a, b):
    return lax.dot_general(
        a, b, (((1,), (1,)), ((), ())), preferred_element_type=jnp.float32
    )


def fold(s, op):
    return op(s.reshape(s.shape[0] // 8, 8, s.shape[1]), axis=0)


def kernel(
    nz,
    nx,
    q_hbm,
    v_hbm,
    ids_hbm,
    neg_hbm,
    nlq_hbm,
    tab_hbm,
    loss_ref,
    qg_ref,
    vg_ref,
    ag,
    ids_ref,
    tab_ref,
    nlq_ref,
    q_all,
    cand,
    cand_t,
    offs,
    off_b,
    gat,
    scores,
    probs,
    probs2,
    cgrad,
    part,
    part_in,
    stat,
    stat_in,
    d2d,
    d2d_in,
    itm,
    itm_in,
    rs,
    rs_in,
    red,
    in_sem,
    q_sem,
    cand_sem,
    off_sem,
    stat_sem,
    part_sem,
    d2d_sem,
    itm_sem,
    rs_sem,
    ag_sem,
):
    rows, width = qg_ref.shape
    neg_rows = ag.shape[0]
    shard = rows + neg_rows
    tall = 4 * shard
    nyh = 2
    groups = nyh * nx
    cut = neg_rows // groups
    order = pair_order(nz)
    pos = {r: i for i, r in enumerate(order)}
    pairs = nz // 2
    early = max(1, pairs // 2)
    ahead = max(0, pairs - 2)

    g = lax.axis_index("grp")
    d = lax.axis_index("dev")
    yh, x = g // nx, g % nx
    z, yl, c = d // 4, (d // 2) % 2, d % 2

    def at(zz, dyl, dc):
        return zz * 4 + ((yl + dyl) % 2) * 2 + (c + dc) % 2

    def grp_at(dyh, dx):
        return ((yh + dyh) % 2) * nx + (x + dx) % nx

    def z_dev(r):
        return (g, at((z + r) % nz, 0, r))

    def distance(dyh, dx, dyl):
        return min(dx, nx - dx) + (1 if dyl else 2 * dyh)

    plane = [
        (dyh, dx, dyl) for dyl in range(2) for dyh in range(nyh) for dx in range(nx)
    ]
    far_first = sorted(plane, key=lambda t: -distance(*t))

    def mirror(dyh, dx, dyl):
        return plane.index((dyh, (nx - dx) % nx, dyl))

    started = []

    def push(src, dst, sems, i, device):
        copy = pltpu.make_async_remote_copy(
            src_ref=src,
            dst_ref=dst,
            send_sem=sems.at[0, i],
            recv_sem=sems.at[1, i],
            device_id=device,
            device_id_type=MESH,
        )
        copy.start()
        started.append(copy)
        return copy

    def rows_of(start, size):
        return pl.ds(start, size)

    loads = [
        pltpu.make_async_copy(q_hbm, q_all.at[rows_of(0, rows)], in_sem.at[0]),
        pltpu.make_async_copy(v_hbm, cand.at[rows_of(0, rows)], in_sem.at[1]),
        pltpu.make_async_copy(neg_hbm, cand.at[rows_of(rows, neg_rows)], in_sem.at[2]),
        pltpu.make_async_copy(ids_hbm, ids_ref, in_sem.at[3]),
        pltpu.make_async_copy(tab_hbm, tab_ref, in_sem.at[4]),
        pltpu.make_async_copy(nlq_hbm, nlq_ref, in_sem.at[5]),
    ]
    for load in loads:
        load.start()

    core_mate = (g, at(z, 0, 1))
    y_mate = (g, at(z, 1, 0))
    y_wrap = (grp_at(1, 0), at(z, 1, 0))
    peers = [z_dev(r) for r in range(1, nz)]
    peers += [(g, at(z, j // 2, j % 2)) for j in (1, 2, 3)]
    peers += [y_wrap]
    peers += [
        (grp_at(dyh, dx), at(z, dyl, 1))
        for dyh, dx, dyl in plane
        if (dyh, dx) != (0, 0)
    ]
    barrier = pltpu.get_barrier_semaphore()
    for peer in peers:
        pl.semaphore_signal(barrier, inc=1, device_id=peer, device_id_type=MESH)
    pl.semaphore_wait(barrier, len(peers))
    for load in loads[:3]:
        load.wait()

    q_copies = {}
    mid = nz // 2
    direct = min(2, mid)

    def forward(held, step, side):
        new = (held - step) % nz
        first, size, i = 0, rows, new
        if new == mid:
            first, size, i = side * rows // 2, rows // 2, mid + side * (nz - mid)
        q_copies[i] = push(
            q_all.at[rows_of(pos[held] * rows + first, size)],
            q_all.at[rows_of(pos[new] * rows + first, size)],
            q_sem,
            i,
            z_dev(step % nz),
        )

    reached = set()

    def reach(k):
        if k in reached:
            return
        reached.add(k)
        for i in (k, nz if k == mid else nz - k):
            q_copies[i].wait_recv()
        if k == direct:
            for far in range(direct + 1, mid + 1):
                forward(k, k - far, 0)
                forward(nz - k, far - k, 1)

    for k in range(1, direct + 1):
        forward(0, -k, 0)
        forward(0, k, 1)

    def shift(lo, size, j, i, device):
        return push(
            cand.at[rows_of(lo, size)],
            cand.at[rows_of(j * shard + lo, size)],
            cand_sem,
            i,
            device,
        )

    cut_at = rows + DIRECT
    y_copies = [
        shift(0, cut_at, 2, 0, y_mate),
        shift(cut_at, shard - cut_at, 2, 1, y_wrap),
    ]
    mate_copy = shift(0, shard, 1, 2, core_mate)

    for load in loads[3:]:
        load.wait()

    def look(i, carry):
        entry = ids_ref[d * rows + i]
        row = tab_ref[pl.ds(lax.shift_right_logical(entry, 7), 1), :]
        lane = lax.broadcasted_iota(jnp.int32, (1, LANES), 1)
        gat[pl.ds(i, 1), :] = jnp.where(lane == (entry & 127), row, 0.0)
        return carry

    lax.fori_loop(0, rows, look, 0, unroll=8)
    offs[0, 0:1, :] = jnp.sum(gat[...].T, axis=0, keepdims=True)
    offs[0, 1 : 1 + neg_rows // LANES, :] = nlq_ref[...]
    off_copies = {}
    for j in (1, 2, 3):
        off_copies[j] = push(
            offs.at[0], offs.at[j], off_sem, j, (g, at(z, j // 2, j % 2))
        )

    eye = lax.broadcasted_iota(jnp.int32, (rows, rows), 0) == lax.broadcasted_iota(
        jnp.int32, (rows, rows), 1
    )
    own = {}

    def prepare(j):
        for k in range(shard // LANES):
            lo = j * shard + k * LANES
            cand_t[:, lo : lo + LANES] = cand[lo : lo + LANES, :].T
        if j:
            off_copies[j].wait_recv()
        for k in range(shard // LANES):
            lo = j * shard + k * LANES
            line = jnp.broadcast_to(offs[j, k : k + 1, :], (LANES, LANES))
            off_b[lo : lo + LANES, :] = line.T

    def score(p, lo, size):
        scaled = q_all[2 * p * rows : (2 * p + 2) * rows, :] * jnp.bfloat16(SCALE)
        ob = off_b[lo : lo + size, :]
        s = dot_nt(cand[lo : lo + size, :], scaled) - jnp.concatenate([ob, ob], axis=1)
        if p == 0 and lo == 0:
            corner = s[:rows, :rows]
            own["score"] = jnp.sum(jnp.where(eye, corner, 0.0), axis=0, keepdims=True)
            corner = jnp.where(eye, MASKED, corner)
            s = jnp.concatenate(
                [jnp.concatenate([corner, s[:rows, rows:]], axis=1), s[rows:]], axis=0
            )
        scores[p, lo : lo + size, :] = s
        return jnp.max(fold(s, jnp.max), axis=0, keepdims=True)

    def weigh(p, lo, size, top):
        total = jnp.zeros((8, 2 * rows), jnp.float32)
        for at_row in range(lo, lo + size, LANES):
            e = jnp.exp(scores[p, at_row : at_row + LANES, :] - top)
            probs[p, at_row : at_row + LANES, :] = e.astype(jnp.bfloat16)
            total = total + fold(e, jnp.sum)
        return jnp.sum(total, axis=0, keepdims=True)

    def pull(p, lo, size):
        return jnp.dot(
            cand_t[:, lo : lo + size],
            probs[p, lo : lo + size, :],
            preferred_element_type=jnp.float32,
        )

    stat_copies = []
    far_peers = sorted(range(1, nz), key=lambda r: -min(r, nz - r))

    def tell(p, top, total):
        if p == 0:
            own["top"] = top[:, :rows]
            mixed = jnp.maximum(own["top"], own["score"])
            own_total = total[:, :rows] * jnp.exp(own["top"] - mixed) + jnp.exp(
                own["score"] - mixed
            )
            top = jnp.concatenate([mixed, top[:, rows:]], axis=1)
            total = jnp.concatenate([own_total, total[:, rows:]], axis=1)
        both = jnp.concatenate([top, total], axis=0)
        stat[p] = both
        stat_in[0, p] = both
        for r in far_peers:
            s = nz - r
            stat_copies.append(
                push(stat.at[p], stat_in.at[s, p], stat_sem, s * pairs + p, z_dev(r))
            )

    def stats_of(block, s):
        i = pos[(block - s) % nz]
        both = stat_in[s, i // 2, :, (i % 2) * rows : (i % 2 + 1) * rows]
        return both[0:1], both[1:2]

    def keep(p, qp):
        for h in range(2):
            part[2 * p + h] = qp[:, h * rows : (h + 1) * rows].astype(jnp.bfloat16)

    half = 2 * shard
    prepare(0)
    mate_copy.wait_recv()
    prepare(1)
    tops, totals, ratios = [], [], []
    for p in range(early):
        reach(p + 1)
        tops.append(score(p, 0, half))
        totals.append(weigh(p, 0, half, tops[p]))
        if p == 0:
            if early > 1:
                reach(2)
            for copy in y_copies:
                copy.wait_recv()
            relay = push(
                cand.at[rows_of(2 * shard, shard)],
                cand.at[rows_of(3 * shard, shard)],
                cand_sem,
                3,
                core_mate,
            )
    prepare(2)
    relay.wait_recv()
    prepare(3)
    for p in range(early):
        top = jnp.maximum(tops[p], score(p, half, half))
        total = weigh(p, half, half, top)
        ratios.append(jnp.exp(tops[p] - top))
        tell(p, top, ratios[p] * totals[p] + total)
        if p == 0 and early < pairs:
            reach(early + 1)
    for p in range(early, pairs):
        reach(p + 1)
        top = score(p, 0, tall)
        total = weigh(p, 0, tall, top)
        tell(p, top, total)
    for p in reversed(range(pairs)):
        if p < early:
            keep(p, ratios[p] * pull(p, 0, half) + pull(p, half, half))
        else:
            keep(p, pull(p, 0, tall))

    part_copies = {}
    for r in reversed(order):
        if r:
            back = nz - r
            part_copies[back] = push(
                part.at[pos[r]], part_in.at[back], part_sem, back, z_dev(r)
            )
    for copy in stat_copies:
        copy.wait_recv()
    own_score = own["score"]
    norms = []
    for r in order:
        tops_r, totals_r = zip(*(stats_of(r, s) for s in range(nz)))
        tops_r = jnp.concatenate(tops_r, axis=0)
        totals_r = jnp.concatenate(totals_r, axis=0)
        best = jnp.max(tops_r, axis=0, keepdims=True)
        mass = jnp.sum(totals_r * jnp.exp(tops_r - best), axis=0, keepdims=True)
        norms.append(best + jnp.log(mass))
    log_norm = norms[pos[0]]
    loss_ref[...] = log_norm - own_score
    own_term = jnp.exp(own_score - log_norm) - 1.0

    def weigh_again(j, slot):
        for p in range(pairs):
            norm = jnp.concatenate(norms[2 * p : 2 * p + 2], axis=1)
            for lo in range(0, shard, LANES):
                at_row = j * shard + lo
                e = jnp.exp(scores[p, at_row : at_row + LANES, :] - norm)
                probs2[slot, lo : lo + LANES, 2 * p * rows : (2 * p + 2) * rows] = (
                    e.astype(jnp.bfloat16)
                )

    d2d_copies, rs_copies = {}, {}

    def exchange(dyl):
        d2d_copies[dyl].wait_recv()
        whole = cgrad[dyl] + d2d_in[dyl].astype(jnp.float32)
        rs[dyl] = whole[rows:].astype(jnp.bfloat16)
        for dyh, dx, dy in far_first:
            if dy == dyl:
                target = grp_at(dyh, dx)
                i = mirror(dyh, dx, dy)
                rs_copies[i] = push(
                    rs.at[dyl, rows_of(pl.multiple_of(target * cut, cut), cut)],
                    rs_in.at[i],
                    rs_sem,
                    i,
                    (target, at(z, dyl, 1)),
                )
        if dyl:
            itm[...] = whole[:rows].astype(jnp.bfloat16)
            return push(itm, itm_in, itm_sem, 0, y_mate)
        cgrad[0, 0:rows, :] = whole[:rows]

    for turn, j in enumerate((3, 2, 1, 0)):
        weigh_again(j, turn % 2)
        grad = SCALE * jnp.dot(
            probs2[turn % 2], q_all[...], preferred_element_type=jnp.float32
        )
        if j % 2:
            i = j // 2
            d2d[i] = grad.astype(jnp.bfloat16)
            d2d_copies[i] = push(d2d.at[i], d2d_in.at[i], d2d_sem, i, core_mate)
        else:
            cgrad[j // 2] = grad
        if j == 1:
            itm_copy = exchange(1)
    exchange(0)

    own_rows = rows_of(pl.multiple_of(g * cut, cut), cut)
    summed = jnp.zeros((cut, width), jnp.float32)
    for i in range(len(plane)):
        rs_copies[i].wait_recv()
        summed = summed + rs_in[i].astype(jnp.float32)
    red[...] = summed.astype(jnp.bfloat16)
    ag_copies = {}
    for dyh, dx, dyl in far_first:
        if dyl == 0:
            i = mirror(dyh, dx, 0)
            ag_copies[i] = push(
                red, ag.at[own_rows], ag_sem, i, (grp_at(dyh, dx), at(z, 0, 1))
            )

    acc = own_term * cand_t[:, 0:rows].astype(jnp.float32)
    for r in range(nz):
        if r:
            part_copies[r].wait_recv()
            piece = part_in[r]
        else:
            piece = part[pos[0]]
        share = jnp.exp((stats_of(0, r)[0] if r else own["top"]) - log_norm)
        acc = acc + share * piece.astype(jnp.float32)
    qg_ref[...] = (SCALE * acc).T

    itm_copy.wait_recv()
    column = jnp.broadcast_to(own_term, (rows, rows)).T
    column = jnp.concatenate([column] * (width // rows), axis=1)
    vg_ref[...] = (
        cgrad[0, 0:rows, :]
        + itm_in[...].astype(jnp.float32)
        + SCALE * column * q_all[0:rows, :].astype(jnp.float32)
    )

    for i in ag_copies:
        ag_copies[i].wait_recv()
    for copy in started:
        copy.wait_send()


def emit(loss_in, qg_in, vg_in, ng_in, loss_ref, qg_ref, vg_ref, ng_ref):
    loss_ref[...] = loss_in[...]
    qg_ref[...] = qg_in[...]
    vg_ref[...] = vg_in[...]
    ng_ref[...] = ng_in[...].astype(jnp.float32)


def local(queries, items, item_ids, neg_embed, neg_logq, logq_table, *, nz, nx):
    rows, width = queries.shape
    neg_rows = neg_embed.shape[0]
    shard = rows + neg_rows
    tall = 4 * shard
    groups = 2 * nx
    cut = neg_rows // groups
    pairs = nz // 2
    f32, bf16 = jnp.float32, jnp.bfloat16
    dma = pltpu.SemaphoreType.DMA
    vmem = pl.BlockSpec(memory_space=pltpu.VMEM)
    away = pl.BlockSpec(memory_space=pl.ANY)
    table = logq_table.reshape(-1, LANES)
    neg_lines = neg_logq.reshape(-1, LANES)
    results = pl.pallas_call(
        functools.partial(kernel, nz, nx),
        out_shape=(
            jax.ShapeDtypeStruct((1, rows), f32),
            jax.ShapeDtypeStruct((rows, width), f32),
            jax.ShapeDtypeStruct((rows, width), f32),
            jax.ShapeDtypeStruct((neg_rows, width), bf16),
        ),
        in_specs=[away] * 6,
        out_specs=(vmem, vmem, vmem, vmem),
        scratch_shapes=[
            pltpu.SMEM(item_ids.shape, jnp.int32),
            pltpu.VMEM(table.shape, f32),
            pltpu.VMEM(neg_lines.shape, f32),
            pltpu.VMEM((nz * rows, width), bf16),
            pltpu.VMEM((tall, width), bf16),
            pltpu.VMEM((width, tall), bf16),
            pltpu.VMEM((4, 8, LANES), f32),
            pltpu.VMEM((tall, LANES), f32),
            pltpu.VMEM((rows, LANES), f32),
            pltpu.VMEM((pairs, tall, 2 * rows), f32),
            pltpu.VMEM((pairs, tall, 2 * rows), bf16),
            pltpu.VMEM((2, shard, nz * rows), bf16),
            pltpu.VMEM((2, shard, width), f32),
            pltpu.VMEM((nz, width, rows), bf16),
            pltpu.VMEM((nz, width, rows), bf16),
            pltpu.VMEM((pairs, 2, 2 * rows), f32),
            pltpu.VMEM((nz, pairs, 2, 2 * rows), f32),
            pltpu.VMEM((2, shard, width), bf16),
            pltpu.VMEM((2, shard, width), bf16),
            pltpu.VMEM((rows, width), bf16),
            pltpu.VMEM((rows, width), bf16),
            pltpu.VMEM((2, neg_rows, width), bf16),
            pltpu.VMEM((2 * groups, cut, width), bf16),
            pltpu.VMEM((cut, width), bf16),
            dma((6,)),
            dma((2, nz + 1)),
            dma((2, 4)),
            dma((2, 4)),
            dma((2, nz * pairs)),
            dma((2, nz)),
            dma((2, 2)),
            dma((2, 1)),
            dma((2, 2 * groups)),
            dma((2, 2 * groups)),
        ],
        compiler_params=pltpu.CompilerParams(
            collective_id=0, has_side_effects=True, vmem_limit_bytes=60 << 20
        ),
    )(queries, items, item_ids, neg_embed, neg_lines, table)
    loss, qg, vg, ng = pl.pallas_call(
        emit,
        out_shape=(
            jax.ShapeDtypeStruct((1, rows), f32),
            jax.ShapeDtypeStruct((rows, width), f32),
            jax.ShapeDtypeStruct((rows, width), f32),
            jax.ShapeDtypeStruct((neg_rows, width), f32),
        ),
        in_specs=[vmem] * 4,
        out_specs=(vmem, vmem, vmem, vmem),
    )(*results)
    return loss.reshape(rows), qg, vg, ng


def solution(mesh):
    return jax.shard_map(
        functools.partial(
            local, nz=mesh.shape["dev"] // 4, nx=mesh.shape["grp"] // 2
        ),
        mesh=mesh,
        in_specs=(
            P(("grp", "dev"), None),
            P(("grp", "dev"), None),
            P("grp"),
            P("dev", None),
            P("dev"),
            P(),
        ),
        out_specs=(
            P(("grp", "dev")),
            P(("grp", "dev"), None),
            P(("grp", "dev"), None),
            P("dev", None),
        ),
        check_vma=False,
    )
```

```python
import functools

import jax
import jax.numpy as jnp
from jax import lax
from jax.experimental import pallas as pl
from jax.experimental.pallas import tpu as pltpu
from jax.sharding import PartitionSpec as P

MESH = pl.DeviceIdType.MESH
SCALE = 0.25
MASKED = -1e30
LANES = 128
DIRECT = 192


def pair_order(nz):
    order = [0, 1]
    for r in range(1, nz // 2):
        order += [nz - r, r + 1]
    return order


def dot_nt(a, b):
    return lax.dot_general(
        a, b, (((1,), (1,)), ((), ())), preferred_element_type=jnp.float32
    )


def fold(s, op):
    return op(s.reshape(s.shape[0] // 8, 8, s.shape[1]), axis=0)


def kernel(
    nz,
    nx,
    q_hbm,
    v_hbm,
    ids_hbm,
    neg_hbm,
    nlq_hbm,
    tab_hbm,
    loss_ref,
    qg_ref,
    vg_ref,
    ag,
    ids_ref,
    tab_ref,
    nlq_ref,
    q_all,
    cand,
    cand_t,
    offs,
    off_b,
    gat,
    scores,
    probs,
    probs2,
    cgrad,
    part,
    part_in,
    stat,
    stat_in,
    d2d,
    d2d_in,
    itm,
    itm_in,
    rs,
    rs_in,
    red,
    in_sem,
    q_sem,
    cand_sem,
    off_sem,
    stat_sem,
    part_sem,
    d2d_sem,
    itm_sem,
    rs_sem,
    ag_sem,
):
    rows, width = qg_ref.shape
    neg_rows = ag.shape[0]
    shard = rows + neg_rows
    tall = 4 * shard
    nyh = 2
    groups = nyh * nx
    cut = neg_rows // groups
    order = pair_order(nz)
    pos = {r: i for i, r in enumerate(order)}
    pairs = mid = nz // 2

    g = lax.axis_index("grp")
    d = lax.axis_index("dev")
    yh, x = g // nx, g % nx
    z, yl, c = d // 4, (d // 2) % 2, d % 2

    def at(zz, dyl, dc):
        return zz * 4 + ((yl + dyl) % 2) * 2 + (c + dc) % 2

    def grp_at(dyh, dx):
        return ((yh + dyh) % 2) * nx + (x + dx) % nx

    def z_dev(r):
        zz = (z + r) % nz
        return (g, at(zz, 0, z + zz + z // mid + zz // mid))

    def distance(dyh, dx, dyl):
        return min(dx, nx - dx) + (1 if dyl else 2 * dyh)

    plane = [
        (dyh, dx, dyl) for dyl in range(2) for dyh in range(nyh) for dx in range(nx)
    ]
    far_first = sorted(plane, key=lambda t: -distance(*t))

    def mirror(dyh, dx, dyl):
        return plane.index((dyh, (nx - dx) % nx, dyl))

    started = []

    def push(src, dst, sems, i, device):
        copy = pltpu.make_async_remote_copy(
            src_ref=src,
            dst_ref=dst,
            send_sem=sems.at[0, i],
            recv_sem=sems.at[1, i],
            device_id=device,
            device_id_type=MESH,
        )
        copy.start()
        started.append(copy)
        return copy

    def rows_of(start, size):
        return pl.ds(start, size)

    loads = [
        pltpu.make_async_copy(q_hbm, q_all.at[rows_of(0, rows)], in_sem.at[0]),
        pltpu.make_async_copy(v_hbm, cand.at[rows_of(0, rows)], in_sem.at[1]),
        pltpu.make_async_copy(neg_hbm, cand.at[rows_of(rows, neg_rows)], in_sem.at[2]),
        pltpu.make_async_copy(ids_hbm, ids_ref, in_sem.at[3]),
        pltpu.make_async_copy(tab_hbm, tab_ref, in_sem.at[4]),
        pltpu.make_async_copy(nlq_hbm, nlq_ref, in_sem.at[5]),
    ]
    for load in loads:
        load.start()

    core_mate = (g, at(z, 0, 1))
    y_mate = (g, at(z, 1, 0))
    y_wrap = (grp_at(1, 0), at(z, 1, 0))
    peers = [z_dev(r) for r in range(1, nz)]
    peers += [(g, at(z, j // 2, j % 2)) for j in (1, 2, 3)]
    peers += [y_wrap]
    peers += [
        (grp_at(dyh, dx), at(z, dyl, 1))
        for dyh, dx, dyl in plane
        if (dyh, dx) != (0, 0)
    ]
    barrier = pltpu.get_barrier_semaphore()
    for peer in peers:
        pl.semaphore_signal(barrier, inc=1, device_id=peer, device_id_type=MESH)
    pl.semaphore_wait(barrier, len(peers))
    for load in loads[:3]:
        load.wait()

    q_copies = {}
    direct = min(2, mid)

    def forward(held, step, side):
        new = (held - step) % nz
        first, size, i = 0, rows, new
        if new == mid:
            first, size, i = side * rows // 2, rows // 2, mid + side * (nz - mid)
        q_copies[i] = push(
            q_all.at[rows_of(pos[held] * rows + first, size)],
            q_all.at[rows_of(pos[new] * rows + first, size)],
            q_sem,
            i,
            z_dev(step % nz),
        )

    reached = set()

    def reach(k):
        if k in reached:
            return
        reached.add(k)
        for i in (k, nz if k == mid else nz - k):
            q_copies[i].wait_recv()
        if k == direct:
            for far in range(direct + 1, mid + 1):
                forward(k, k - far, 0)
                forward(nz - k, far - k, 1)

    for k in range(1, direct + 1):
        forward(0, -k, 0)
        forward(0, k, 1)

    def shift(lo, size, j, i, device):
        return push(
            cand.at[rows_of(lo, size)],
            cand.at[rows_of(j * shard + lo, size)],
            cand_sem,
            i,
            device,
        )

    cut_at = rows + DIRECT
    y_copies = [
        shift(0, cut_at, 2, 0, y_mate),
        shift(cut_at, shard - cut_at, 2, 1, y_wrap),
    ]
    mate_copy = shift(0, shard, 1, 2, core_mate)

    for load in loads[3:]:
        load.wait()

    def look(i, carry):
        entry = ids_ref[d * rows + i]
        row = tab_ref[pl.ds(lax.shift_right_logical(entry, 7), 1), :]
        lane = lax.broadcasted_iota(jnp.int32, (1, LANES), 1)
        gat[pl.ds(i, 1), :] = jnp.where(lane == (entry & 127), row, 0.0)
        return carry

    lax.fori_loop(0, rows, look, 0, unroll=8)
    offs[0, 0:1, :] = jnp.sum(gat[...].T, axis=0, keepdims=True)
    offs[0, 1 : 1 + neg_rows // LANES, :] = nlq_ref[...]
    off_copies = {}
    for j in (1, 2, 3):
        off_copies[j] = push(
            offs.at[0], offs.at[j], off_sem, j, (g, at(z, j // 2, j % 2))
        )

    eye = lax.broadcasted_iota(jnp.int32, (rows, rows), 0) == lax.broadcasted_iota(
        jnp.int32, (rows, rows), 1
    )
    own = {}

    def prepare(j):
        for k in range(shard // LANES):
            lo = j * shard + k * LANES
            cand_t[:, lo : lo + LANES] = cand[lo : lo + LANES, :].T
        if j:
            off_copies[j].wait_recv()
        for k in range(shard // LANES):
            lo = j * shard + k * LANES
            line = jnp.broadcast_to(offs[j, k : k + 1, :], (LANES, LANES))
            off_b[lo : lo + LANES, :] = line.T

    def score(p, lo, size):
        scaled = q_all[2 * p * rows : (2 * p + 2) * rows, :] * jnp.bfloat16(SCALE)
        top = jnp.full((8, 2 * rows), MASKED, jnp.float32)
        for at_row in range(lo, lo + size, 256):
            ob = off_b[at_row : at_row + 256, :]
            s = dot_nt(cand[at_row : at_row + 256, :], scaled)
            s = s - jnp.concatenate([ob, ob], axis=1)
            if p == 0 and at_row == 0:
                corner = s[:rows, :rows]
                own["score"] = jnp.sum(
                    jnp.where(eye, corner, 0.0), axis=0, keepdims=True
                )
                corner = jnp.where(eye, MASKED, corner)
                line = jnp.concatenate([corner, s[:rows, rows:]], axis=1)
                s = jnp.concatenate([line, s[rows:]], axis=0) if 256 > rows else line
            scores[p, at_row : at_row + 256, :] = s
            top = jnp.maximum(top, fold(s, jnp.max))
        return jnp.max(top, axis=0, keepdims=True)

    def weigh(p, lo, size, top):
        total = jnp.zeros((8, 2 * rows), jnp.float32)
        for at_row in range(lo, lo + size, LANES):
            e = jnp.exp(scores[p, at_row : at_row + LANES, :] - top)
            probs[p, at_row : at_row + LANES, :] = e.astype(jnp.bfloat16)
            total = total + fold(e, jnp.sum)
        return jnp.sum(total, axis=0, keepdims=True)

    def pull(p, lo, size):
        return jnp.dot(
            cand_t[:, lo : lo + size],
            probs[p, lo : lo + size, :],
            preferred_element_type=jnp.float32,
        )

    stat_copies = []
    far_peers = sorted(range(1, nz), key=lambda r: -min(r, nz - r))

    def tell(p, top, total):
        if p == 0:
            own["top"] = top[:, :rows]
            mixed = jnp.maximum(own["top"], own["score"])
            own_total = total[:, :rows] * jnp.exp(own["top"] - mixed) + jnp.exp(
                own["score"] - mixed
            )
            top = jnp.concatenate([mixed, top[:, rows:]], axis=1)
            total = jnp.concatenate([own_total, total[:, rows:]], axis=1)
        both = jnp.concatenate([top, total], axis=0)
        stat[p] = both
        stat_in[0, p] = both
        for r in far_peers:
            s = nz - r
            stat_copies.append(
                push(stat.at[p], stat_in.at[s, p], stat_sem, s * pairs + p, z_dev(r))
            )

    def stats_of(block, s):
        i = pos[(block - s) % nz]
        both = stat_in[s, i // 2, :, (i % 2) * rows : (i % 2 + 1) * rows]
        return both[0:1], both[1:2]

    def keep(p, qp):
        for h in range(2):
            part[2 * p + h] = qp[:, h * rows : (h + 1) * rows].astype(jnp.bfloat16)

    half = 2 * shard
    prepare(0)
    mate_copy.wait_recv()
    prepare(1)
    reach(1)
    first_top = score(0, 0, half)
    first_total = weigh(0, 0, half, first_top)
    for copy in y_copies:
        copy.wait_recv()
    relay = push(
        cand.at[rows_of(2 * shard, shard)],
        cand.at[rows_of(3 * shard, shard)],
        cand_sem,
        3,
        core_mate,
    )
    prepare(2)
    if pairs > 1:
        reach(2)
    relay.wait_recv()
    prepare(3)
    top = jnp.maximum(first_top, score(0, half, half))
    total = weigh(0, half, half, top)
    ratio = jnp.exp(first_top - top)
    tell(0, top, ratio * first_total + total)
    for p in range(1, pairs):
        reach(p + 1)
        top = score(p, 0, tall)
        total = weigh(p, 0, tall, top)
        tell(p, top, total)
    for p in reversed(range(pairs)):
        if p:
            keep(p, pull(p, 0, tall))
        else:
            keep(p, ratio * pull(p, 0, half) + pull(p, half, half))

    for copy in stat_copies:
        copy.wait_recv()
    part_copies = {}
    for r in reversed(order):
        if r:
            back = nz - r
            part_copies[back] = push(
                part.at[pos[r]], part_in.at[back], part_sem, back, z_dev(r)
            )
    own_score = own["score"]
    norms = []
    for r in order:
        tops_r, totals_r = zip(*(stats_of(r, s) for s in range(nz)))
        tops_r = jnp.concatenate(tops_r, axis=0)
        totals_r = jnp.concatenate(totals_r, axis=0)
        best = jnp.max(tops_r, axis=0, keepdims=True)
        mass = jnp.sum(totals_r * jnp.exp(tops_r - best), axis=0, keepdims=True)
        norms.append(best + jnp.log(mass))
    log_norm = norms[pos[0]]
    loss_ref[...] = log_norm - own_score
    own_term = jnp.exp(own_score - log_norm) - 1.0

    def weigh_again(j, slot):
        for p in range(pairs):
            norm = jnp.concatenate(norms[2 * p : 2 * p + 2], axis=1)
            for lo in range(0, shard, LANES):
                at_row = j * shard + lo
                e = jnp.exp(scores[p, at_row : at_row + LANES, :] - norm)
                probs2[slot, lo : lo + LANES, 2 * p * rows : (2 * p + 2) * rows] = (
                    e.astype(jnp.bfloat16)
                )

    d2d_copies, rs_copies = {}, {}

    def exchange(dyl):
        d2d_copies[dyl].wait_recv()
        whole = cgrad[dyl] + d2d_in[dyl].astype(jnp.float32)
        rs[dyl] = whole[rows:].astype(jnp.bfloat16)
        for dyh, dx, dy in far_first:
            if dy == dyl:
                target = grp_at(dyh, dx)
                i = mirror(dyh, dx, dy)
                rs_copies[i] = push(
                    rs.at[dyl, rows_of(pl.multiple_of(target * cut, cut), cut)],
                    rs_in.at[i],
                    rs_sem,
                    i,
                    (target, at(z, dyl, 1)),
                )
        if dyl:
            itm[...] = whole[:rows].astype(jnp.bfloat16)
            return push(itm, itm_in, itm_sem, 0, y_mate)
        cgrad[0, 0:rows, :] = whole[:rows]

    for turn, j in enumerate((3, 2, 1, 0)):
        weigh_again(j, turn % 2)
        grad = SCALE * jnp.dot(
            probs2[turn % 2], q_all[...], preferred_element_type=jnp.float32
        )
        if j % 2:
            i = j // 2
            d2d[i] = grad.astype(jnp.bfloat16)
            d2d_copies[i] = push(d2d.at[i], d2d_in.at[i], d2d_sem, i, core_mate)
        else:
            cgrad[j // 2] = grad
        if j == 1:
            itm_copy = exchange(1)
    exchange(0)

    own_rows = rows_of(pl.multiple_of(g * cut, cut), cut)
    summed = jnp.zeros((cut, width), jnp.float32)
    for i in range(len(plane)):
        rs_copies[i].wait_recv()
        summed = summed + rs_in[i].astype(jnp.float32)
    red[...] = summed.astype(jnp.bfloat16)
    ag_copies = {}
    for dyh, dx, dyl in far_first:
        if dyl == 0:
            i = mirror(dyh, dx, 0)
            ag_copies[i] = push(
                red, ag.at[own_rows], ag_sem, i, (grp_at(dyh, dx), at(z, 0, 1))
            )

    acc = own_term * cand_t[:, 0:rows].astype(jnp.float32)
    for r in range(nz):
        if r:
            part_copies[r].wait_recv()
            piece = part_in[r]
        else:
            piece = part[pos[0]]
        share = jnp.exp((stats_of(0, r)[0] if r else own["top"]) - log_norm)
        acc = acc + share * piece.astype(jnp.float32)
    qg_ref[...] = (SCALE * acc).T

    itm_copy.wait_recv()
    column = jnp.broadcast_to(own_term, (rows, rows)).T
    column = jnp.concatenate([column] * (width // rows), axis=1)
    vg_ref[...] = (
        cgrad[0, 0:rows, :]
        + itm_in[...].astype(jnp.float32)
        + SCALE * column * q_all[0:rows, :].astype(jnp.float32)
    )

    for i in ag_copies:
        ag_copies[i].wait_recv()
    for copy in started:
        copy.wait_send()


def emit(loss_in, qg_in, vg_in, ng_in, loss, qg, vg, ng, wide, sem):
    copies = [
        pltpu.make_async_copy(qg_in, qg, sem.at[0]),
        pltpu.make_async_copy(vg_in, vg, sem.at[1]),
        pltpu.make_async_copy(loss_in, loss, sem.at[2]),
    ]
    for copy in copies:
        copy.start()
    size = ng_in.shape[0] // 2
    for i in range(2):
        span = pl.ds(i * size, size)
        wide[span, :] = ng_in[span, :].astype(jnp.float32)
        copy = pltpu.make_async_copy(wide.at[span], ng.at[span], sem.at[3 + i])
        copy.start()
        copies.append(copy)
    for copy in copies:
        copy.wait()


def local(queries, items, item_ids, neg_embed, neg_logq, logq_table, *, nz, nx):
    rows, width = queries.shape
    neg_rows = neg_embed.shape[0]
    shard = rows + neg_rows
    tall = 4 * shard
    groups = 2 * nx
    cut = neg_rows // groups
    pairs = nz // 2
    f32, bf16 = jnp.float32, jnp.bfloat16
    dma = pltpu.SemaphoreType.DMA
    vmem = pl.BlockSpec(memory_space=pltpu.VMEM)
    away = pl.BlockSpec(memory_space=pl.ANY)
    table = logq_table.reshape(-1, LANES)
    neg_lines = neg_logq.reshape(-1, LANES)
    results = pl.pallas_call(
        functools.partial(kernel, nz, nx),
        out_shape=(
            pltpu.VMEM((1, rows), f32),
            pltpu.VMEM((rows, width), f32),
            pltpu.VMEM((rows, width), f32),
            pltpu.VMEM((neg_rows, width), bf16),
        ),
        in_specs=[away] * 6,
        out_specs=(vmem, vmem, vmem, vmem),
        scratch_shapes=[
            pltpu.SMEM(item_ids.shape, jnp.int32),
            pltpu.VMEM(table.shape, f32),
            pltpu.VMEM(neg_lines.shape, f32),
            pltpu.VMEM((nz * rows, width), bf16),
            pltpu.VMEM((tall, width), bf16),
            pltpu.VMEM((width, tall), bf16),
            pltpu.VMEM((4, 8, LANES), f32),
            pltpu.VMEM((tall, LANES), f32),
            pltpu.VMEM((rows, LANES), f32),
            pltpu.VMEM((pairs, tall, 2 * rows), f32),
            pltpu.VMEM((pairs, tall, 2 * rows), bf16),
            pltpu.VMEM((2, shard, nz * rows), bf16),
            pltpu.VMEM((2, shard, width), f32),
            pltpu.VMEM((nz, width, rows), bf16),
            pltpu.VMEM((nz, width, rows), bf16),
            pltpu.VMEM((pairs, 2, 2 * rows), f32),
            pltpu.VMEM((nz, pairs, 2, 2 * rows), f32),
            pltpu.VMEM((2, shard, width), bf16),
            pltpu.VMEM((2, shard, width), bf16),
            pltpu.VMEM((rows, width), bf16),
            pltpu.VMEM((rows, width), bf16),
            pltpu.VMEM((2, neg_rows, width), bf16),
            pltpu.VMEM((2 * groups, cut, width), bf16),
            pltpu.VMEM((cut, width), bf16),
            dma((6,)),
            dma((2, nz + 1)),
            dma((2, 4)),
            dma((2, 4)),
            dma((2, nz * pairs)),
            dma((2, nz)),
            dma((2, 2)),
            dma((2, 1)),
            dma((2, 2 * groups)),
            dma((2, 2 * groups)),
        ],
        compiler_params=pltpu.CompilerParams(
            collective_id=0, has_side_effects=True, vmem_limit_bytes=60 << 20
        ),
    )(queries, items, item_ids, neg_embed, neg_lines, table)
    loss, qg, vg, ng = pl.pallas_call(
        emit,
        out_shape=(
            jax.ShapeDtypeStruct((1, rows), f32),
            jax.ShapeDtypeStruct((rows, width), f32),
            jax.ShapeDtypeStruct((rows, width), f32),
            jax.ShapeDtypeStruct((neg_rows, width), f32),
        ),
        in_specs=[vmem] * 4,
        out_specs=(away, away, away, away),
        scratch_shapes=[pltpu.VMEM((neg_rows, width), f32), dma((5,))],
    )(*(pltpu.with_memory_space_constraint(r, pltpu.VMEM) for r in results))
    return loss.reshape(rows), qg, vg, ng


def solution(mesh):
    return jax.shard_map(
        functools.partial(
            local, nz=mesh.shape["dev"] // 4, nx=mesh.shape["grp"] // 2
        ),
        mesh=mesh,
        in_specs=(
            P(("grp", "dev"), None),
            P(("grp", "dev"), None),
            P("grp"),
            P("dev", None),
            P("dev"),
            P(),
        ),
        out_specs=(
            P(("grp", "dev")),
            P(("grp", "dev"), None),
            P(("grp", "dev"), None),
            P("dev", None),
        ),
        check_vma=False,
    )
```

```python
import functools

import jax
import jax.numpy as jnp
from jax import lax
from jax.experimental import pallas as pl
from jax.experimental.pallas import tpu as pltpu
from jax.sharding import PartitionSpec as P

MESH = pl.DeviceIdType.MESH
SCALE = 0.25
MASKED = -1e30
LANES = 128
DIRECT = 192


def pair_order(nz):
    order = [0, nz // 2]
    for r in range(1, nz // 2):
        order += [r, nz - r]
    return order


def dot_nt(a, b):
    return lax.dot_general(
        a, b, (((1,), (1,)), ((), ())), preferred_element_type=jnp.float32
    )


def fold(s, op):
    return op(s.reshape(s.shape[0] // 8, 8, s.shape[1]), axis=0)


def kernel(
    nz,
    nx,
    q_hbm,
    v_hbm,
    ids_hbm,
    neg_hbm,
    nlq_hbm,
    tab_hbm,
    loss_ref,
    qg_ref,
    vg_ref,
    ag,
    ids_ref,
    tab_ref,
    nlq_ref,
    q_all,
    cand,
    cand_t,
    offs,
    off_b,
    gat,
    scores,
    probs,
    cgrad,
    part,
    part_in,
    stat,
    stat_in,
    d2d,
    d2d_in,
    itm,
    itm_in,
    rs,
    rs_in,
    red,
    in_sem,
    q_sem,
    cand_sem,
    off_sem,
    stat_sem,
    part_sem,
    d2d_sem,
    itm_sem,
    rs_sem,
    ag_sem,
):
    rows, width = qg_ref.shape
    neg_rows = ag.shape[0]
    shard = rows + neg_rows
    tall = 4 * shard
    nyh = 2
    groups = nyh * nx
    cut = neg_rows // groups
    order = pair_order(nz)
    pos = {r: i for i, r in enumerate(order)}
    pairs = mid = nz // 2

    g = lax.axis_index("grp")
    d = lax.axis_index("dev")
    yh, x = g // nx, g % nx
    z, yl, c = d // 4, (d // 2) % 2, d % 2

    def at(zz, dyl, dc):
        return zz * 4 + ((yl + dyl) % 2) * 2 + (c + dc) % 2

    def grp_at(dyh, dx):
        return ((yh + dyh) % 2) * nx + (x + dx) % nx

    def z_dev(r):
        zz = (z + r) % nz
        return (g, at(zz, 0, z + zz + z // mid + zz // mid))

    def distance(dyh, dx, dyl):
        return min(dx, nx - dx) + (1 if dyl else 2 * dyh)

    plane = [
        (dyh, dx, dyl) for dyl in range(2) for dyh in range(nyh) for dx in range(nx)
    ]
    far_first = sorted(plane, key=lambda t: -distance(*t))

    def mirror(dyh, dx, dyl):
        return plane.index((dyh, (nx - dx) % nx, dyl))

    started = []

    def push(src, dst, sems, i, device):
        copy = pltpu.make_async_remote_copy(
            src_ref=src,
            dst_ref=dst,
            send_sem=sems.at[0, i],
            recv_sem=sems.at[1, i],
            device_id=device,
            device_id_type=MESH,
        )
        copy.start()
        started.append(copy)
        return copy

    def rows_of(start, size):
        return pl.ds(start, size)

    def lanes_of(p):
        return slice(2 * p * rows, (2 * p + 2) * rows)

    core_mate = (g, at(z, 0, 1))
    y_mate = (g, at(z, 1, 0))
    y_wrap = (grp_at(1, 0), at(z, 1, 0))
    peers = [z_dev(r) for r in range(1, nz)]
    peers += [(g, at(z, j // 2, j % 2)) for j in (1, 2, 3)]
    peers += [y_wrap]
    peers += [
        (grp_at(dyh, dx), at(z, dyl, 1))
        for dyh, dx, dyl in plane
        if (dyh, dx) != (0, 0)
    ]
    barrier = pltpu.get_barrier_semaphore()
    for peer in peers:
        pl.semaphore_signal(barrier, inc=1, device_id=peer, device_id_type=MESH)
    loads = [
        pltpu.make_async_copy(q_hbm, q_all.at[rows_of(0, rows)], in_sem.at[0]),
        pltpu.make_async_copy(v_hbm, cand.at[rows_of(0, rows)], in_sem.at[1]),
        pltpu.make_async_copy(neg_hbm, cand.at[rows_of(rows, neg_rows)], in_sem.at[2]),
        pltpu.make_async_copy(ids_hbm, ids_ref, in_sem.at[3]),
        pltpu.make_async_copy(tab_hbm, tab_ref, in_sem.at[4]),
        pltpu.make_async_copy(nlq_hbm, nlq_ref, in_sem.at[5]),
    ]
    for load in loads:
        load.start()
    pl.semaphore_wait(barrier, len(peers))
    for load in loads[:3]:
        load.wait()

    q_copies = {}
    direct = min(2, mid)

    def forward(held, step, side):
        new = (held - step) % nz
        first, size, i = 0, rows, new
        if new == mid:
            first, size, i = side * rows // 2, rows // 2, mid + side * (nz - mid)
        q_copies[i] = push(
            q_all.at[rows_of(pos[held] * rows + first, size)],
            q_all.at[rows_of(pos[new] * rows + first, size)],
            q_sem,
            i,
            z_dev(step % nz),
        )

    reached = set()

    def reach(k):
        if k in reached:
            return
        reached.add(k)
        for i in (k, nz if k == mid else nz - k):
            q_copies[i].wait_recv()
        if k == direct:
            for far in range(3, mid + 1):
                forward(k, k - far, 0)
                forward(nz - k, far - k, 1)

    for k in [k for k in (2, 1) if k <= mid]:
        forward(0, -k, 0)
        forward(0, k, 1)

    def shift(lo, size, j, i, device):
        return push(
            cand.at[rows_of(lo, size)],
            cand.at[rows_of(j * shard + lo, size)],
            cand_sem,
            i,
            device,
        )

    cut_at = rows + DIRECT
    y_copies = [
        shift(0, cut_at, 2, 0, y_mate),
        shift(cut_at, shard - cut_at, 2, 1, y_wrap),
    ]
    mate_copy = shift(0, shard, 1, 2, core_mate)

    for load in loads[3:]:
        load.wait()

    def look(i, carry):
        entry = ids_ref[d * rows + i]
        row = tab_ref[pl.ds(lax.shift_right_logical(entry, 7), 1), :]
        lane = lax.broadcasted_iota(jnp.int32, (1, LANES), 1)
        gat[pl.ds(i, 1), :] = jnp.where(lane == (entry & 127), row, 0.0)
        return carry

    lax.fori_loop(0, rows, look, 0, unroll=8)
    offs[0, 0:1, :] = jnp.sum(gat[...].T, axis=0, keepdims=True)
    offs[0, 1 : 1 + neg_rows // LANES, :] = nlq_ref[...]
    off_copies = {}
    for j in (1, 2, 3):
        off_copies[j] = push(
            offs.at[0], offs.at[j], off_sem, j, (g, at(z, j // 2, j % 2))
        )

    eye = lax.broadcasted_iota(jnp.int32, (rows, rows), 0) == lax.broadcasted_iota(
        jnp.int32, (rows, rows), 1
    )
    own = {}

    def prepare(j):
        for k in range(shard // LANES):
            lo = j * shard + k * LANES
            cand_t[:, lo : lo + LANES] = cand[lo : lo + LANES, :].T
        if j:
            off_copies[j].wait_recv()
        for k in range(shard // LANES):
            lo = j * shard + k * LANES
            line = jnp.broadcast_to(offs[j, k : k + 1, :], (LANES, LANES))
            off_b[lo : lo + LANES, :] = line.T

    def score(p, lo, size):
        scaled = q_all[2 * p * rows : (2 * p + 2) * rows, :] * jnp.bfloat16(SCALE)
        top = jnp.full((8, 2 * rows), MASKED, jnp.float32)
        for at_row in range(lo, lo + size, 256):
            ob = off_b[at_row : at_row + 256, :]
            s = dot_nt(cand[at_row : at_row + 256, :], scaled)
            s = s - jnp.concatenate([ob, ob], axis=1)
            if p == 0 and at_row == 0:
                corner = s[:rows, :rows]
                own["score"] = jnp.sum(
                    jnp.where(eye, corner, 0.0), axis=0, keepdims=True
                )
                corner = jnp.where(eye, MASKED, corner)
                line = jnp.concatenate([corner, s[:rows, rows:]], axis=1)
                s = jnp.concatenate([line, s[rows:]], axis=0) if 256 > rows else line
            scores[p, at_row : at_row + 256, :] = s
            top = jnp.maximum(top, fold(s, jnp.max))
        return jnp.max(top, axis=0, keepdims=True)

    def weigh(p, lo, size, top):
        total = jnp.zeros((8, 2 * rows), jnp.float32)
        for at_row in range(lo, lo + size, LANES):
            e = jnp.exp(scores[p, at_row : at_row + LANES, :] - top)
            probs[at_row : at_row + LANES, lanes_of(p)] = e.astype(jnp.bfloat16)
            total = total + fold(e, jnp.sum)
        return jnp.sum(total, axis=0, keepdims=True)

    def pull(p, lo, size):
        return jnp.dot(
            cand_t[:, lo : lo + size],
            probs[lo : lo + size, lanes_of(p)],
            preferred_element_type=jnp.float32,
        )

    stat_copies = {}
    far_peers = sorted(range(1, nz), key=lambda r: -min(r, nz - r))

    def tell(p, top, total):
        if p == 0:
            own["top"] = top[:, :rows]
            mixed = jnp.maximum(own["top"], own["score"])
            own_total = total[:, :rows] * jnp.exp(own["top"] - mixed) + jnp.exp(
                own["score"] - mixed
            )
            top = jnp.concatenate([mixed, top[:, rows:]], axis=1)
            total = jnp.concatenate([own_total, total[:, rows:]], axis=1)
        both = jnp.concatenate([top, total], axis=0)
        stat[p] = both
        stat_in[0, p] = both
        for r in far_peers:
            s = nz - r
            stat_copies[s, p] = push(
                stat.at[p], stat_in.at[s, p], stat_sem, s * pairs + p, z_dev(r)
            )

    def stats_of(block, s):
        i = pos[(block - s) % nz]
        both = stat_in[s, i // 2, :, (i % 2) * rows : (i % 2 + 1) * rows]
        return both[0:1], both[1:2]

    def keep(p, qp):
        for h in range(2):
            part[2 * p + h] = qp[:, h * rows : (h + 1) * rows].astype(jnp.bfloat16)

    half = 2 * shard
    prepare(0)
    mate_copy.wait_recv()
    prepare(1)
    turns = [p for p in (2, 1, 3) if p < pairs] + [0]
    lead = turns[0]
    reach(lead or mid)
    first_top = score(lead, 0, half)
    first_total = weigh(lead, 0, half, first_top)
    for copy in y_copies:
        copy.wait_recv()
    relay = push(
        cand.at[rows_of(2 * shard, shard)],
        cand.at[rows_of(3 * shard, shard)],
        cand_sem,
        3,
        core_mate,
    )
    prepare(2)
    relay.wait_recv()
    prepare(3)
    top = jnp.maximum(first_top, score(lead, half, half))
    total = weigh(lead, half, half, top)
    ratio = jnp.exp(first_top - top)
    tell(lead, top, ratio * first_total + total)
    for p in turns[1:]:
        reach(p or mid)
        top = score(p, 0, tall)
        total = weigh(p, 0, tall, top)
        tell(p, top, total)
    for p in reversed(range(pairs)):
        if p != lead:
            keep(p, pull(p, 0, tall))
        else:
            keep(p, ratio * pull(p, 0, half) + pull(p, half, half))

    own_score = own["score"]
    norms = {}

    def settle(p):
        for r in order[2 * p : 2 * p + 2]:
            for s in range(1, nz):
                copy = stat_copies.pop((s, pos[(r - s) % nz] // 2), None)
                if copy is not None:
                    copy.wait_recv()
        for r in order[2 * p : 2 * p + 2]:
            tops_r, totals_r = zip(*(stats_of(r, s) for s in range(nz)))
            tops_r = jnp.concatenate(tops_r, axis=0)
            totals_r = jnp.concatenate(totals_r, axis=0)
            best = jnp.max(tops_r, axis=0, keepdims=True)
            mass = jnp.sum(totals_r * jnp.exp(tops_r - best), axis=0, keepdims=True)
            norms[r] = best + jnp.log(mass)

    def weigh_again(p, first, last):
        norm = jnp.concatenate([norms[r] for r in order[2 * p : 2 * p + 2]], axis=1)
        for at_row in range(first * shard, last * shard, LANES):
            e = jnp.exp(scores[p, at_row : at_row + LANES, :] - norm)
            probs[at_row : at_row + LANES, lanes_of(p)] = e.astype(jnp.bfloat16)

    sooner = [p for p in (2, 3) if p < pairs]
    later = [p for p in (1, 0) if p < pairs]
    for p in sooner:
        settle(p)
        weigh_again(p, 0, 4)
    for p in later:
        settle(p)
    part_copies = {}
    for r in reversed(order):
        if r:
            back = nz - r
            part_copies[back] = push(
                part.at[pos[r]], part_in.at[back], part_sem, back, z_dev(r)
            )
    log_norm = norms[0]
    loss_ref[...] = log_norm - own_score
    own_term = jnp.exp(own_score - log_norm) - 1.0

    d2d_copies, rs_copies = {}, {}

    def exchange(dyl):
        d2d_copies[dyl].wait_recv()
        whole = cgrad[dyl] + d2d_in[dyl].astype(jnp.float32)
        rs[dyl] = whole[rows:].astype(jnp.bfloat16)
        for dyh, dx, dy in far_first:
            if dy == dyl:
                target = grp_at(dyh, dx)
                i = mirror(dyh, dx, dy)
                rs_copies[i] = push(
                    rs.at[dyl, rows_of(pl.multiple_of(target * cut, cut), cut)],
                    rs_in.at[i],
                    rs_sem,
                    i,
                    (target, at(z, dyl, 1)),
                )
        if dyl:
            itm[...] = whole[:rows].astype(jnp.bfloat16)
            return push(itm, itm_in, itm_sem, 0, y_mate)
        cgrad[0, 0:rows, :] = whole[:rows]

    for j in (3, 1, 2, 0):
        for p in later:
            weigh_again(p, j, j + 1)
        grad = jnp.dot(
            probs[j * shard : (j + 1) * shard, :],
            q_all[...],
            preferred_element_type=jnp.float32,
        )
        grad = SCALE * grad
        if j % 2:
            i = j // 2
            d2d[i] = grad.astype(jnp.bfloat16)
            d2d_copies[i] = push(d2d.at[i], d2d_in.at[i], d2d_sem, i, core_mate)
        else:
            cgrad[j // 2] = grad
        if j == 2:
            itm_copy = exchange(1)
    exchange(0)

    own_rows = rows_of(pl.multiple_of(g * cut, cut), cut)
    summed = jnp.zeros((cut, width), jnp.float32)
    for i in range(len(plane)):
        rs_copies[i].wait_recv()
        summed = summed + rs_in[i].astype(jnp.float32)
    red[...] = summed.astype(jnp.bfloat16)
    ag_copies = {}
    for dyh, dx, dyl in far_first:
        if dyl == 0:
            i = mirror(dyh, dx, 0)
            ag_copies[i] = push(
                red, ag.at[own_rows], ag_sem, i, (grp_at(dyh, dx), at(z, 0, 1))
            )

    acc = own_term * cand_t[:, 0:rows].astype(jnp.float32)
    for r in range(nz):
        if r:
            part_copies[r].wait_recv()
            piece = part_in[r]
        else:
            piece = part[pos[0]]
        share = jnp.exp((stats_of(0, r)[0] if r else own["top"]) - log_norm)
        acc = acc + share * piece.astype(jnp.float32)
    qg_ref[...] = (SCALE * acc).T

    itm_copy.wait_recv()
    column = jnp.broadcast_to(own_term, (rows, rows)).T
    column = jnp.concatenate([column] * (width // rows), axis=1)
    vg_ref[...] = (
        cgrad[0, 0:rows, :]
        + itm_in[...].astype(jnp.float32)
        + SCALE * column * q_all[0:rows, :].astype(jnp.float32)
    )

    for i in ag_copies:
        ag_copies[i].wait_recv()
    for copy in started:
        copy.wait_send()


def emit(loss_in, qg_in, vg_in, ng_in, loss, qg, vg, ng, wide, sem):
    copies = [
        pltpu.make_async_copy(qg_in, qg, sem.at[0]),
        pltpu.make_async_copy(vg_in, vg, sem.at[1]),
        pltpu.make_async_copy(loss_in, loss, sem.at[2]),
    ]
    for copy in copies:
        copy.start()
    size = ng_in.shape[0] // 2
    for i in range(2):
        span = pl.ds(i * size, size)
        wide[span, :] = ng_in[span, :].astype(jnp.float32)
        copy = pltpu.make_async_copy(wide.at[span], ng.at[span], sem.at[3 + i])
        copy.start()
        copies.append(copy)
    for copy in copies:
        copy.wait()


def local(queries, items, item_ids, neg_embed, neg_logq, logq_table, *, nz, nx):
    rows, width = queries.shape
    neg_rows = neg_embed.shape[0]
    shard = rows + neg_rows
    tall = 4 * shard
    groups = 2 * nx
    cut = neg_rows // groups
    pairs = nz // 2
    f32, bf16 = jnp.float32, jnp.bfloat16
    dma = pltpu.SemaphoreType.DMA
    vmem = pl.BlockSpec(memory_space=pltpu.VMEM)
    away = pl.BlockSpec(memory_space=pl.ANY)
    table = logq_table.reshape(-1, LANES)
    neg_lines = neg_logq.reshape(-1, LANES)
    results = pl.pallas_call(
        functools.partial(kernel, nz, nx),
        out_shape=(
            pltpu.VMEM((1, rows), f32),
            pltpu.VMEM((rows, width), f32),
            pltpu.VMEM((rows, width), f32),
            pltpu.VMEM((neg_rows, width), bf16),
        ),
        in_specs=[away] * 6,
        out_specs=(vmem, vmem, vmem, vmem),
        scratch_shapes=[
            pltpu.SMEM(item_ids.shape, jnp.int32),
            pltpu.VMEM(table.shape, f32),
            pltpu.VMEM(neg_lines.shape, f32),
            pltpu.VMEM((nz * rows, width), bf16),
            pltpu.VMEM((tall, width), bf16),
            pltpu.VMEM((width, tall), bf16),
            pltpu.VMEM((4, 8, LANES), f32),
            pltpu.VMEM((tall, LANES), f32),
            pltpu.VMEM((rows, LANES), f32),
            pltpu.VMEM((pairs, tall, 2 * rows), f32),
            pltpu.VMEM((tall, nz * rows), bf16),
            pltpu.VMEM((2, shard, width), f32),
            pltpu.VMEM((nz, width, rows), bf16),
            pltpu.VMEM((nz, width, rows), bf16),
            pltpu.VMEM((pairs, 2, 2 * rows), f32),
            pltpu.VMEM((nz, pairs, 2, 2 * rows), f32),
            pltpu.VMEM((2, shard, width), bf16),
            pltpu.VMEM((2, shard, width), bf16),
            pltpu.VMEM((rows, width), bf16),
            pltpu.VMEM((rows, width), bf16),
            pltpu.VMEM((2, neg_rows, width), bf16),
            pltpu.VMEM((2 * groups, cut, width), bf16),
            pltpu.VMEM((cut, width), bf16),
            dma((6,)),
            dma((2, nz + 1)),
            dma((2, 4)),
            dma((2, 4)),
            dma((2, nz * pairs)),
            dma((2, nz)),
            dma((2, 2)),
            dma((2, 1)),
            dma((2, 2 * groups)),
            dma((2, 2 * groups)),
        ],
        compiler_params=pltpu.CompilerParams(
            collective_id=0, has_side_effects=True, vmem_limit_bytes=60 << 20
        ),
    )(queries, items, item_ids, neg_embed, neg_lines, table)
    loss, qg, vg, ng = pl.pallas_call(
        emit,
        out_shape=(
            jax.ShapeDtypeStruct((1, rows), f32),
            jax.ShapeDtypeStruct((rows, width), f32),
            jax.ShapeDtypeStruct((rows, width), f32),
            jax.ShapeDtypeStruct((neg_rows, width), f32),
        ),
        in_specs=[vmem] * 4,
        out_specs=(away, away, away, away),
        scratch_shapes=[pltpu.VMEM((neg_rows, width), f32), dma((5,))],
    )(*(pltpu.with_memory_space_constraint(r, pltpu.VMEM) for r in results))
    return loss.reshape(rows), qg, vg, ng


def solution(mesh):
    return jax.shard_map(
        functools.partial(
            local, nz=mesh.shape["dev"] // 4, nx=mesh.shape["grp"] // 2
        ),
        mesh=mesh,
        in_specs=(
            P(("grp", "dev"), None),
            P(("grp", "dev"), None),
            P("grp"),
            P("dev", None),
            P("dev"),
            P(),
        ),
        out_specs=(
            P(("grp", "dev")),
            P(("grp", "dev"), None),
            P(("grp", "dev"), None),
            P("dev", None),
        ),
        check_vma=False,
    )
```

```python
import functools

import jax
import jax.numpy as jnp
from jax import lax
from jax.experimental import pallas as pl
from jax.experimental.pallas import tpu as pltpu
from jax.sharding import PartitionSpec as P

MESH = pl.DeviceIdType.MESH
SCALE = 0.25
MASKED = -1e30
LANES = 128
DIRECT = 192


def pair_order(nz):
    order = [0, nz // 2]
    for r in range(1, nz // 2):
        order += [r, nz - r]
    return order


def dot_nt(a, b):
    return lax.dot_general(
        a, b, (((1,), (1,)), ((), ())), preferred_element_type=jnp.float32
    )


def fold(s, op):
    return op(s.reshape(s.shape[0] // 8, 8, s.shape[1]), axis=0)


def kernel(
    nz,
    nx,
    q_hbm,
    v_hbm,
    ids_hbm,
    neg_hbm,
    nlq_hbm,
    tab_hbm,
    loss_ref,
    qg_ref,
    vg_ref,
    ag,
    ids_ref,
    tab_ref,
    nlq_ref,
    q_all,
    cand,
    cand_t,
    offs,
    off_b,
    gat,
    scores,
    probs,
    cgrad,
    part,
    part_in,
    stat,
    stat_in,
    d2d,
    d2d_in,
    itm,
    itm_in,
    rs,
    rs_in,
    red,
    in_sem,
    q_sem,
    cand_sem,
    off_sem,
    stat_sem,
    part_sem,
    d2d_sem,
    itm_sem,
    rs_sem,
    ag_sem,
):
    rows, width = qg_ref.shape
    neg_rows = ag.shape[0]
    shard = rows + neg_rows
    tall = 4 * shard
    nyh = 2
    groups = nyh * nx
    cut = neg_rows // groups
    order = pair_order(nz)
    pos = {r: i for i, r in enumerate(order)}
    pairs = mid = nz // 2

    g = lax.axis_index("grp")
    d = lax.axis_index("dev")
    yh, x = g // nx, g % nx
    z, yl, c = d // 4, (d // 2) % 2, d % 2

    def at(zz, dyl, dc):
        return zz * 4 + ((yl + dyl) % 2) * 2 + (c + dc) % 2

    def grp_at(dyh, dx):
        return ((yh + dyh) % 2) * nx + (x + dx) % nx

    def z_dev(r):
        zz = (z + r) % nz
        return (g, at(zz, 0, z + zz + z // mid + zz // mid))

    def distance(dyh, dx, dyl):
        return min(dx, nx - dx) + (1 if dyl else 2 * dyh)

    plane = [
        (dyh, dx, dyl) for dyl in range(2) for dyh in range(nyh) for dx in range(nx)
    ]
    far_first = sorted(plane, key=lambda t: -distance(*t))

    def mirror(dyh, dx, dyl):
        return plane.index((dyh, (nx - dx) % nx, dyl))

    started = []

    def push(src, dst, sems, i, device):
        copy = pltpu.make_async_remote_copy(
            src_ref=src,
            dst_ref=dst,
            send_sem=sems.at[0, i],
            recv_sem=sems.at[1, i],
            device_id=device,
            device_id_type=MESH,
        )
        copy.start()
        started.append(copy)
        return copy

    def rows_of(start, size):
        return pl.ds(start, size)

    def lanes_of(p):
        return slice(2 * p * rows, (2 * p + 2) * rows)

    core_mate = (g, at(z, 0, 1))
    y_mate = (g, at(z, 1, 0))
    y_wrap = (grp_at(1, 0), at(z, 1, 0))
    peers = [z_dev(r) for r in range(1, nz)]
    peers += [(g, at(z, j // 2, j % 2)) for j in (1, 2, 3)]
    peers += [y_wrap]
    peers += [
        (grp_at(dyh, dx), at(z, dyl, 1))
        for dyh, dx, dyl in plane
        if (dyh, dx) != (0, 0)
    ]
    barrier = pltpu.get_barrier_semaphore()
    for peer in peers:
        pl.semaphore_signal(barrier, inc=1, device_id=peer, device_id_type=MESH)
    loads = [
        pltpu.make_async_copy(q_hbm, q_all.at[rows_of(0, rows)], in_sem.at[0]),
        pltpu.make_async_copy(v_hbm, cand.at[rows_of(0, rows)], in_sem.at[1]),
        pltpu.make_async_copy(neg_hbm, cand.at[rows_of(rows, neg_rows)], in_sem.at[2]),
        pltpu.make_async_copy(ids_hbm, ids_ref, in_sem.at[3]),
        pltpu.make_async_copy(tab_hbm, tab_ref, in_sem.at[4]),
        pltpu.make_async_copy(nlq_hbm, nlq_ref, in_sem.at[5]),
    ]
    for load in loads:
        load.start()
    pl.semaphore_wait(barrier, len(peers))
    for load in loads[:3]:
        load.wait()

    q_copies = {}
    direct = min(2, mid)

    def forward(held, step, side):
        new = (held - step) % nz
        first, size, i = 0, rows, new
        if new == mid:
            first, size, i = side * rows // 2, rows // 2, mid + side * (nz - mid)
        q_copies[i] = push(
            q_all.at[rows_of(pos[held] * rows + first, size)],
            q_all.at[rows_of(pos[new] * rows + first, size)],
            q_sem,
            i,
            z_dev(step % nz),
        )

    reached = set()

    def reach(k):
        if k in reached:
            return
        reached.add(k)
        for i in (k, nz if k == mid else nz - k):
            q_copies[i].wait_recv()
        if k == direct:
            for far in range(3, mid + 1):
                forward(k, k - far, 0)
                forward(nz - k, far - k, 1)

    for k in [k for k in (2, 1) if k <= mid]:
        forward(0, -k, 0)
        forward(0, k, 1)

    def shift(lo, size, j, i, device):
        return push(
            cand.at[rows_of(lo, size)],
            cand.at[rows_of(j * shard + lo, size)],
            cand_sem,
            i,
            device,
        )

    cut_at = rows + DIRECT
    y_copies = [
        shift(0, cut_at, 2, 0, y_mate),
        shift(cut_at, shard - cut_at, 2, 1, y_wrap),
    ]
    mate_copy = shift(0, shard, 1, 2, core_mate)

    for load in loads[3:]:
        load.wait()

    def look(i, carry):
        entry = ids_ref[d * rows + i]
        row = tab_ref[pl.ds(lax.shift_right_logical(entry, 7), 1), :]
        lane = lax.broadcasted_iota(jnp.int32, (1, LANES), 1)
        gat[pl.ds(i, 1), :] = jnp.where(lane == (entry & 127), row, 0.0)
        return carry

    lax.fori_loop(0, rows, look, 0, unroll=8)
    offs[0, 0:1, :] = jnp.sum(gat[...].T, axis=0, keepdims=True)
    offs[0, 1 : 1 + neg_rows // LANES, :] = nlq_ref[...]
    off_copies = {}
    for j in (1, 2, 3):
        off_copies[j] = push(
            offs.at[0], offs.at[j], off_sem, j, (g, at(z, j // 2, j % 2))
        )

    eye = lax.broadcasted_iota(jnp.int32, (rows, rows), 0) == lax.broadcasted_iota(
        jnp.int32, (rows, rows), 1
    )
    own = {}

    def flip(j):
        for k in range(shard // LANES):
            lo = j * shard + k * LANES
            cand_t[:, lo : lo + LANES] = cand[lo : lo + LANES, :].T

    def spread(j):
        if j:
            off_copies[j].wait_recv()
        for k in range(shard // LANES):
            lo = j * shard + k * LANES
            line = jnp.broadcast_to(offs[j, k : k + 1, :], (LANES, LANES))
            off_b[lo : lo + LANES, :] = line.T

    def score(p, lo, size):
        scaled = q_all[2 * p * rows : (2 * p + 2) * rows, :] * jnp.bfloat16(SCALE)
        top = jnp.full((8, 2 * rows), MASKED, jnp.float32)
        for at_row in range(lo, lo + size, 256):
            ob = off_b[at_row : at_row + 256, :]
            s = dot_nt(cand[at_row : at_row + 256, :], scaled)
            s = s - jnp.concatenate([ob, ob], axis=1)
            if p == 0 and at_row == 0:
                corner = s[:rows, :rows]
                own["score"] = jnp.sum(
                    jnp.where(eye, corner, 0.0), axis=0, keepdims=True
                )
                corner = jnp.where(eye, MASKED, corner)
                line = jnp.concatenate([corner, s[:rows, rows:]], axis=1)
                s = jnp.concatenate([line, s[rows:]], axis=0) if 256 > rows else line
            scores[p, at_row : at_row + 256, :] = s
            top = jnp.maximum(top, fold(s, jnp.max))
        return jnp.max(top, axis=0, keepdims=True)

    def weigh(p, lo, size, top):
        total = jnp.zeros((8, 2 * rows), jnp.float32)
        for at_row in range(lo, lo + size, LANES):
            e = jnp.exp(scores[p, at_row : at_row + LANES, :] - top)
            probs[at_row : at_row + LANES, lanes_of(p)] = e.astype(jnp.bfloat16)
            total = total + fold(e, jnp.sum)
        return jnp.sum(total, axis=0, keepdims=True)

    def pull(p, lo, size):
        return jnp.dot(
            cand_t[:, lo : lo + size],
            probs[lo : lo + size, lanes_of(p)],
            preferred_element_type=jnp.float32,
        )

    stat_copies = {}
    far_peers = sorted(range(1, nz), key=lambda r: -min(r, nz - r))

    def tell(p, top, total):
        if p == 0:
            own["top"] = top[:, :rows]
            mixed = jnp.maximum(own["top"], own["score"])
            own_total = total[:, :rows] * jnp.exp(own["top"] - mixed) + jnp.exp(
                own["score"] - mixed
            )
            top = jnp.concatenate([mixed, top[:, rows:]], axis=1)
            total = jnp.concatenate([own_total, total[:, rows:]], axis=1)
        both = jnp.concatenate([top, total], axis=0)
        stat[p] = both
        stat_in[0, p] = both
        for r in far_peers:
            s = nz - r
            stat_copies[s, p] = push(
                stat.at[p], stat_in.at[s, p], stat_sem, s * pairs + p, z_dev(r)
            )

    def stats_of(block, s):
        i = pos[(block - s) % nz]
        both = stat_in[s, i // 2, :, (i % 2) * rows : (i % 2 + 1) * rows]
        return both[0:1], both[1:2]

    def keep(p, qp):
        for h in range(2):
            part[2 * p + h] = qp[:, h * rows : (h + 1) * rows].astype(jnp.bfloat16)

    half = 2 * shard
    spread(0)
    flip(0)
    mate_copy.wait_recv()
    flip(1)
    for j in (1, 2, 3):
        spread(j)
    turns = [p for p in (2, 1, 3) if p < pairs] + [0]
    split = turns[: 2 if pairs > 2 else 1]
    tops, totals, ratios = {}, {}, {}

    def first_round(p):
        reach(p or mid)
        tops[p] = score(p, 0, half)
        totals[p] = weigh(p, 0, half, tops[p])

    first_round(split[0])
    for copy in y_copies:
        copy.wait_recv()
    relay = push(
        cand.at[rows_of(2 * shard, shard)],
        cand.at[rows_of(3 * shard, shard)],
        cand_sem,
        3,
        core_mate,
    )
    for p in split[1:]:
        first_round(p)
    relay.wait_recv()
    for p in split:
        top = jnp.maximum(tops[p], score(p, half, half))
        total = weigh(p, half, half, top)
        ratios[p] = jnp.exp(tops[p] - top)
        tell(p, top, ratios[p] * totals[p] + total)
    for p in turns[len(split) :]:
        reach(p or mid)
        top = score(p, 0, tall)
        total = weigh(p, 0, tall, top)
        tell(p, top, total)
    flip(2)
    flip(3)
    for p in range(pairs):
        if p in split:
            keep(p, ratios[p] * pull(p, 0, half) + pull(p, half, half))
        else:
            keep(p, pull(p, 0, tall))

    part_copies = {}
    for r in reversed(order):
        if r:
            back = nz - r
            part_copies[back] = push(
                part.at[pos[r]], part_in.at[back], part_sem, back, z_dev(r)
            )
    own_score = own["score"]
    norms = {}

    def settle(p):
        for r in order[2 * p : 2 * p + 2]:
            for s in range(1, nz):
                copy = stat_copies.pop((s, pos[(r - s) % nz] // 2), None)
                if copy is not None:
                    copy.wait_recv()
        for r in order[2 * p : 2 * p + 2]:
            tops_r, totals_r = zip(*(stats_of(r, s) for s in range(nz)))
            tops_r = jnp.concatenate(tops_r, axis=0)
            totals_r = jnp.concatenate(totals_r, axis=0)
            best = jnp.max(tops_r, axis=0, keepdims=True)
            mass = jnp.sum(totals_r * jnp.exp(tops_r - best), axis=0, keepdims=True)
            norms[r] = best + jnp.log(mass)

    def weigh_again(p, first, last):
        norm = jnp.concatenate([norms[r] for r in order[2 * p : 2 * p + 2]], axis=1)
        for at_row in range(first * shard, last * shard, LANES):
            e = jnp.exp(scores[p, at_row : at_row + LANES, :] - norm)
            probs[at_row : at_row + LANES, lanes_of(p)] = e.astype(jnp.bfloat16)

    sooner = [p for p in (2, 3) if p < pairs]
    later = [p for p in (1, 0) if p < pairs]
    for p in sooner:
        settle(p)
        weigh_again(p, 0, 4)
    for p in later:
        settle(p)
    log_norm = norms[0]
    loss_ref[...] = log_norm - own_score
    own_term = jnp.exp(own_score - log_norm) - 1.0

    d2d_copies, rs_copies = {}, {}

    def exchange(dyl):
        d2d_copies[dyl].wait_recv()
        whole = cgrad[dyl] + d2d_in[dyl].astype(jnp.float32)
        rs[dyl] = whole[rows:].astype(jnp.bfloat16)
        for dyh, dx, dy in far_first:
            if dy == dyl:
                target = grp_at(dyh, dx)
                i = mirror(dyh, dx, dy)
                rs_copies[i] = push(
                    rs.at[dyl, rows_of(pl.multiple_of(target * cut, cut), cut)],
                    rs_in.at[i],
                    rs_sem,
                    i,
                    (target, at(z, dyl, 1)),
                )
        if dyl:
            itm[...] = whole[:rows].astype(jnp.bfloat16)
            return push(itm, itm_in, itm_sem, 0, y_mate)
        cgrad[0, 0:rows, :] = whole[:rows]

    for j in (3, 1, 2, 0):
        for p in later:
            weigh_again(p, j, j + 1)
        grad = jnp.dot(
            probs[j * shard : (j + 1) * shard, :],
            q_all[...],
            preferred_element_type=jnp.float32,
        )
        grad = SCALE * grad
        if j % 2:
            i = j // 2
            d2d[i] = grad.astype(jnp.bfloat16)
            d2d_copies[i] = push(d2d.at[i], d2d_in.at[i], d2d_sem, i, core_mate)
        else:
            cgrad[j // 2] = grad
        if j == 2:
            itm_copy = exchange(1)
    exchange(0)

    own_rows = rows_of(pl.multiple_of(g * cut, cut), cut)
    summed = jnp.zeros((cut, width), jnp.float32)
    for i in range(len(plane)):
        rs_copies[i].wait_recv()
        summed = summed + rs_in[i].astype(jnp.float32)
    red[...] = summed.astype(jnp.bfloat16)
    ag_copies = {}
    for dyh, dx, dyl in far_first:
        if dyl == 0:
            i = mirror(dyh, dx, 0)
            ag_copies[i] = push(
                red, ag.at[own_rows], ag_sem, i, (grp_at(dyh, dx), at(z, 0, 1))
            )

    acc = own_term * cand_t[:, 0:rows].astype(jnp.float32)
    for r in range(nz):
        if r:
            part_copies[r].wait_recv()
            piece = part_in[r]
        else:
            piece = part[pos[0]]
        share = jnp.exp((stats_of(0, r)[0] if r else own["top"]) - log_norm)
        acc = acc + share * piece.astype(jnp.float32)
    qg_ref[...] = (SCALE * acc).T

    itm_copy.wait_recv()
    column = jnp.broadcast_to(own_term, (rows, rows)).T
    column = jnp.concatenate([column] * (width // rows), axis=1)
    vg_ref[...] = (
        cgrad[0, 0:rows, :]
        + itm_in[...].astype(jnp.float32)
        + SCALE * column * q_all[0:rows, :].astype(jnp.float32)
    )

    for i in ag_copies:
        ag_copies[i].wait_recv()
    for copy in started:
        copy.wait_send()


def emit(loss_in, qg_in, vg_in, ng_in, loss, qg, vg, ng, wide, sem):
    copies = [
        pltpu.make_async_copy(qg_in, qg, sem.at[0]),
        pltpu.make_async_copy(vg_in, vg, sem.at[1]),
        pltpu.make_async_copy(loss_in, loss, sem.at[2]),
    ]
    for copy in copies:
        copy.start()
    size = ng_in.shape[0] // 2
    for i in range(2):
        span = pl.ds(i * size, size)
        wide[span, :] = ng_in[span, :].astype(jnp.float32)
        copy = pltpu.make_async_copy(wide.at[span], ng.at[span], sem.at[3 + i])
        copy.start()
        copies.append(copy)
    for copy in copies:
        copy.wait()


def local(queries, items, item_ids, neg_embed, neg_logq, logq_table, *, nz, nx):
    rows, width = queries.shape
    neg_rows = neg_embed.shape[0]
    shard = rows + neg_rows
    tall = 4 * shard
    groups = 2 * nx
    cut = neg_rows // groups
    pairs = nz // 2
    f32, bf16 = jnp.float32, jnp.bfloat16
    dma = pltpu.SemaphoreType.DMA
    vmem = pl.BlockSpec(memory_space=pltpu.VMEM)
    away = pl.BlockSpec(memory_space=pl.ANY)
    table = logq_table.reshape(-1, LANES)
    neg_lines = neg_logq.reshape(-1, LANES)
    results = pl.pallas_call(
        functools.partial(kernel, nz, nx),
        out_shape=(
            pltpu.VMEM((1, rows), f32),
            pltpu.VMEM((rows, width), f32),
            pltpu.VMEM((rows, width), f32),
            pltpu.VMEM((neg_rows, width), bf16),
        ),
        in_specs=[away] * 6,
        out_specs=(vmem, vmem, vmem, vmem),
        scratch_shapes=[
            pltpu.SMEM(item_ids.shape, jnp.int32),
            pltpu.VMEM(table.shape, f32),
            pltpu.VMEM(neg_lines.shape, f32),
            pltpu.VMEM((nz * rows, width), bf16),
            pltpu.VMEM((tall, width), bf16),
            pltpu.VMEM((width, tall), bf16),
            pltpu.VMEM((4, 8, LANES), f32),
            pltpu.VMEM((tall, LANES), f32),
            pltpu.VMEM((rows, LANES), f32),
            pltpu.VMEM((pairs, tall, 2 * rows), f32),
            pltpu.VMEM((tall, nz * rows), bf16),
            pltpu.VMEM((2, shard, width), f32),
            pltpu.VMEM((nz, width, rows), bf16),
            pltpu.VMEM((nz, width, rows), bf16),
            pltpu.VMEM((pairs, 2, 2 * rows), f32),
            pltpu.VMEM((nz, pairs, 2, 2 * rows), f32),
            pltpu.VMEM((2, shard, width), bf16),
            pltpu.VMEM((2, shard, width), bf16),
            pltpu.VMEM((rows, width), bf16),
            pltpu.VMEM((rows, width), bf16),
            pltpu.VMEM((2, neg_rows, width), bf16),
            pltpu.VMEM((2 * groups, cut, width), bf16),
            pltpu.VMEM((cut, width), bf16),
            dma((6,)),
            dma((2, nz + 1)),
            dma((2, 4)),
            dma((2, 4)),
            dma((2, nz * pairs)),
            dma((2, nz)),
            dma((2, 2)),
            dma((2, 1)),
            dma((2, 2 * groups)),
            dma((2, 2 * groups)),
        ],
        compiler_params=pltpu.CompilerParams(
            collective_id=0, has_side_effects=True, vmem_limit_bytes=60 << 20
        ),
    )(queries, items, item_ids, neg_embed, neg_lines, table)
    loss, qg, vg, ng = pl.pallas_call(
        emit,
        out_shape=(
            jax.ShapeDtypeStruct((1, rows), f32),
            jax.ShapeDtypeStruct((rows, width), f32),
            jax.ShapeDtypeStruct((rows, width), f32),
            jax.ShapeDtypeStruct((neg_rows, width), f32),
        ),
        in_specs=[vmem] * 4,
        out_specs=(away, away, away, away),
        scratch_shapes=[pltpu.VMEM((neg_rows, width), f32), dma((5,))],
    )(*(pltpu.with_memory_space_constraint(r, pltpu.VMEM) for r in results))
    return loss.reshape(rows), qg, vg, ng


def solution(mesh):
    return jax.shard_map(
        functools.partial(
            local, nz=mesh.shape["dev"] // 4, nx=mesh.shape["grp"] // 2
        ),
        mesh=mesh,
        in_specs=(
            P(("grp", "dev"), None),
            P(("grp", "dev"), None),
            P("grp"),
            P("dev", None),
            P("dev"),
            P(),
        ),
        out_specs=(
            P(("grp", "dev")),
            P(("grp", "dev"), None),
            P(("grp", "dev"), None),
            P("dev", None),
        ),
        check_vma=False,
    )
```

```python
import functools

import jax
import jax.numpy as jnp
from jax import lax
from jax.experimental import pallas as pl
from jax.experimental.pallas import tpu as pltpu
from jax.sharding import PartitionSpec as P

MESH = pl.DeviceIdType.MESH
SCALE = 0.25
MASKED = -1e30
LANES = 128
DIRECT = 192


def pair_order(nz):
    order = [0, nz // 2]
    for r in range(1, nz // 2):
        order += [r, nz - r]
    return order


def dot_nt(a, b):
    return lax.dot_general(
        a, b, (((1,), (1,)), ((), ())), preferred_element_type=jnp.float32
    )


def fold(s, op):
    return op(s.reshape(s.shape[0] // 8, 8, s.shape[1]), axis=0)


def kernel(
    nz,
    nx,
    q_hbm,
    v_hbm,
    ids_hbm,
    neg_hbm,
    nlq_hbm,
    tab_hbm,
    loss_ref,
    qg_ref,
    vg_ref,
    ag,
    ids_ref,
    tab_ref,
    nlq_ref,
    q_all,
    cand,
    cand_t,
    offs,
    off_b,
    gat,
    scores,
    probs,
    cgrad,
    part,
    part_in,
    stat,
    stat_in,
    d2d,
    d2d_in,
    itm,
    itm_in,
    rs,
    rs_in,
    red,
    in_sem,
    q_sem,
    cand_sem,
    off_sem,
    stat_sem,
    part_sem,
    d2d_sem,
    itm_sem,
    rs_sem,
    ag_sem,
):
    rows, width = qg_ref.shape
    neg_rows = ag.shape[0]
    shard = rows + neg_rows
    tall = 4 * shard
    nyh = 2
    groups = nyh * nx
    cut = neg_rows // groups
    order = pair_order(nz)
    pos = {r: i for i, r in enumerate(order)}
    pairs = mid = nz // 2

    g = lax.axis_index("grp")
    d = lax.axis_index("dev")
    yh, x = g // nx, g % nx
    z, yl, c = d // 4, (d // 2) % 2, d % 2

    def at(zz, dyl, dc):
        return zz * 4 + ((yl + dyl) % 2) * 2 + (c + dc) % 2

    def grp_at(dyh, dx):
        return ((yh + dyh) % 2) * nx + (x + dx) % nx

    def z_dev(r):
        zz = (z + r) % nz
        return (g, at(zz, 0, z + zz + z // mid + zz // mid))

    def distance(dyh, dx, dyl):
        return min(dx, nx - dx) + (1 if dyl else 2 * dyh)

    plane = [
        (dyh, dx, dyl) for dyl in range(2) for dyh in range(nyh) for dx in range(nx)
    ]
    far_first = sorted(plane, key=lambda t: -distance(*t))

    def mirror(dyh, dx, dyl):
        return plane.index((dyh, (nx - dx) % nx, dyl))

    started = []

    def push(src, dst, sems, i, device):
        copy = pltpu.make_async_remote_copy(
            src_ref=src,
            dst_ref=dst,
            send_sem=sems.at[0, i],
            recv_sem=sems.at[1, i],
            device_id=device,
            device_id_type=MESH,
        )
        copy.start()
        started.append(copy)
        return copy

    def rows_of(start, size):
        return pl.ds(start, size)

    def lanes_of(p):
        return slice(2 * p * rows, (2 * p + 2) * rows)

    core_mate = (g, at(z, 0, 1))
    y_mate = (g, at(z, 1, 0))
    y_wrap = (grp_at(1, 0), at(z, 1, 0))
    peers = [z_dev(r) for r in range(1, nz)]
    peers += [(g, at(z, j // 2, j % 2)) for j in (1, 2, 3)]
    peers += [y_wrap]
    peers += [
        (grp_at(dyh, dx), at(z, dyl, 1))
        for dyh, dx, dyl in plane
        if (dyh, dx) != (0, 0)
    ]
    barrier = pltpu.get_barrier_semaphore()
    for peer in peers:
        pl.semaphore_signal(barrier, inc=1, device_id=peer, device_id_type=MESH)
    loads = [
        pltpu.make_async_copy(q_hbm, q_all.at[rows_of(0, rows)], in_sem.at[0]),
        pltpu.make_async_copy(v_hbm, cand.at[rows_of(0, rows)], in_sem.at[1]),
        pltpu.make_async_copy(neg_hbm, cand.at[rows_of(rows, neg_rows)], in_sem.at[2]),
        pltpu.make_async_copy(ids_hbm, ids_ref, in_sem.at[3]),
        pltpu.make_async_copy(tab_hbm, tab_ref, in_sem.at[4]),
        pltpu.make_async_copy(nlq_hbm, nlq_ref, in_sem.at[5]),
    ]
    for load in loads:
        load.start()
    pl.semaphore_wait(barrier, len(peers))
    for load in loads[:3]:
        load.wait()

    q_copies = {}
    direct = min(2, mid)

    def forward(held, step, side):
        new = (held - step) % nz
        first, size, i = 0, rows, new
        if new == mid:
            first, size, i = side * rows // 2, rows // 2, mid + side * (nz - mid)
        q_copies[i] = push(
            q_all.at[rows_of(pos[held] * rows + first, size)],
            q_all.at[rows_of(pos[new] * rows + first, size)],
            q_sem,
            i,
            z_dev(step % nz),
        )

    reached = set()

    def reach(k):
        if k in reached:
            return
        reached.add(k)
        for i in (k, nz if k == mid else nz - k):
            q_copies[i].wait_recv()
        if k == direct:
            for far in range(3, mid + 1):
                forward(k, k - far, 0)
                forward(nz - k, far - k, 1)

    for k in [k for k in (2, 1) if k <= mid]:
        forward(0, -k, 0)
        forward(0, k, 1)

    def shift(lo, size, j, i, device):
        return push(
            cand.at[rows_of(lo, size)],
            cand.at[rows_of(j * shard + lo, size)],
            cand_sem,
            i,
            device,
        )

    cut_at = rows + DIRECT
    y_copies = [
        shift(0, cut_at, 2, 0, y_mate),
        shift(cut_at, shard - cut_at, 2, 1, y_wrap),
    ]
    mate_copy = shift(0, shard, 1, 2, core_mate)

    for load in loads[3:]:
        load.wait()

    def look(i, carry):
        entry = ids_ref[d * rows + i]
        row = tab_ref[pl.ds(lax.shift_right_logical(entry, 7), 1), :]
        lane = lax.broadcasted_iota(jnp.int32, (1, LANES), 1)
        gat[pl.ds(i, 1), :] = jnp.where(lane == (entry & 127), row, 0.0)
        return carry

    lax.fori_loop(0, rows, look, 0, unroll=8)
    offs[0, 0:1, :] = jnp.sum(gat[...].T, axis=0, keepdims=True)
    offs[0, 1 : 1 + neg_rows // LANES, :] = nlq_ref[...]
    off_copies = {}
    for j in (1, 2, 3):
        off_copies[j] = push(
            offs.at[0], offs.at[j], off_sem, j, (g, at(z, j // 2, j % 2))
        )

    eye = lax.broadcasted_iota(jnp.int32, (rows, rows), 0) == lax.broadcasted_iota(
        jnp.int32, (rows, rows), 1
    )
    own = {}

    def flip(j):
        for k in range(shard // LANES):
            lo = j * shard + k * LANES
            cand_t[:, lo : lo + LANES] = cand[lo : lo + LANES, :].T

    def spread(j):
        if j:
            off_copies[j].wait_recv()
        for k in range(shard // LANES):
            lo = j * shard + k * LANES
            line = jnp.broadcast_to(offs[j, k : k + 1, :], (LANES, LANES))
            off_b[lo : lo + LANES, :] = line.T

    def score(p, lo, size):
        scaled = q_all[2 * p * rows : (2 * p + 2) * rows, :] * jnp.bfloat16(SCALE)
        top = jnp.full((8, 2 * rows), MASKED, jnp.float32)
        for at_row in range(lo, lo + size, 256):
            ob = off_b[at_row : at_row + 256, :]
            s = dot_nt(cand[at_row : at_row + 256, :], scaled)
            s = s - jnp.concatenate([ob, ob], axis=1)
            if p == 0 and at_row == 0:
                corner = s[:rows, :rows]
                own["score"] = jnp.sum(
                    jnp.where(eye, corner, 0.0), axis=0, keepdims=True
                )
                corner = jnp.where(eye, MASKED, corner)
                line = jnp.concatenate([corner, s[:rows, rows:]], axis=1)
                s = jnp.concatenate([line, s[rows:]], axis=0) if 256 > rows else line
            scores[p, at_row : at_row + 256, :] = s
            top = jnp.maximum(top, fold(s, jnp.max))
        return jnp.max(top, axis=0, keepdims=True)

    def weigh(p, lo, size, top):
        total = jnp.zeros((8, 2 * rows), jnp.float32)
        for at_row in range(lo, lo + size, LANES):
            e = jnp.exp(scores[p, at_row : at_row + LANES, :] - top)
            probs[at_row : at_row + LANES, lanes_of(p)] = e.astype(jnp.bfloat16)
            total = total + fold(e, jnp.sum)
        return jnp.sum(total, axis=0, keepdims=True)

    def pull(p, lo, size):
        return jnp.dot(
            cand_t[:, lo : lo + size],
            probs[lo : lo + size, lanes_of(p)],
            preferred_element_type=jnp.float32,
        )

    stat_copies = {}
    far_peers = sorted(range(1, nz), key=lambda r: -min(r, nz - r))

    def tell(p, top, total):
        if p == 0:
            own["top"] = top[:, :rows]
            mixed = jnp.maximum(own["top"], own["score"])
            own_total = total[:, :rows] * jnp.exp(own["top"] - mixed) + jnp.exp(
                own["score"] - mixed
            )
            top = jnp.concatenate([mixed, top[:, rows:]], axis=1)
            total = jnp.concatenate([own_total, total[:, rows:]], axis=1)
        both = jnp.concatenate([top, total], axis=0)
        stat[p] = both
        stat_in[0, p] = both
        for r in far_peers:
            s = nz - r
            stat_copies[s, p] = push(
                stat.at[p], stat_in.at[s, p], stat_sem, s * pairs + p, z_dev(r)
            )

    def stats_of(block, s):
        i = pos[(block - s) % nz]
        both = stat_in[s, i // 2, :, (i % 2) * rows : (i % 2 + 1) * rows]
        return both[0:1], both[1:2]

    def keep(p, qp):
        for h in range(2):
            part[2 * p + h] = qp[:, h * rows : (h + 1) * rows].astype(jnp.bfloat16)

    half = 2 * shard
    spread(0)
    flip(0)
    mate_copy.wait_recv()
    flip(1)
    for j in (1, 2, 3):
        spread(j)
    turns = [p for p in (2, 1, 3) if p < pairs] + [0]
    split = turns[: 2 if pairs > 2 else 1]
    tops, totals, ratios = {}, {}, {}

    def first_round(p):
        reach(p or mid)
        tops[p] = score(p, 0, half)
        totals[p] = weigh(p, 0, half, tops[p])

    first_round(split[0])
    relays = []
    for i, (lo, size) in enumerate(((0, cut_at), (cut_at, shard - cut_at))):
        y_copies[i].wait_recv()
        relays.append(
            push(
                cand.at[rows_of(2 * shard + lo, size)],
                cand.at[rows_of(3 * shard + lo, size)],
                cand_sem,
                3 + i,
                core_mate,
            )
        )
    for p in split[1:]:
        first_round(p)
    for relay in relays:
        relay.wait_recv()
    for p in split:
        top = jnp.maximum(tops[p], score(p, half, half))
        total = weigh(p, half, half, top)
        ratios[p] = jnp.exp(tops[p] - top)
        tell(p, top, ratios[p] * totals[p] + total)
    for p in turns[len(split) :]:
        reach(p or mid)
        top = score(p, 0, tall)
        total = weigh(p, 0, tall, top)
        tell(p, top, total)
    flip(2)
    flip(3)
    for p in range(pairs):
        if p in split:
            keep(p, ratios[p] * pull(p, 0, half) + pull(p, half, half))
        else:
            keep(p, pull(p, 0, tall))

    part_copies = {}
    for r in reversed(order):
        if r:
            back = nz - r
            part_copies[back] = push(
                part.at[pos[r]], part_in.at[back], part_sem, back, z_dev(r)
            )
    own_score = own["score"]
    norms = {}

    def settle(p):
        for r in order[2 * p : 2 * p + 2]:
            for s in range(1, nz):
                copy = stat_copies.pop((s, pos[(r - s) % nz] // 2), None)
                if copy is not None:
                    copy.wait_recv()
        for r in order[2 * p : 2 * p + 2]:
            tops_r, totals_r = zip(*(stats_of(r, s) for s in range(nz)))
            tops_r = jnp.concatenate(tops_r, axis=0)
            totals_r = jnp.concatenate(totals_r, axis=0)
            best = jnp.max(tops_r, axis=0, keepdims=True)
            mass = jnp.sum(totals_r * jnp.exp(tops_r - best), axis=0, keepdims=True)
            norms[r] = best + jnp.log(mass)

    def weigh_again(p, first, last):
        norm = jnp.concatenate([norms[r] for r in order[2 * p : 2 * p + 2]], axis=1)
        for at_row in range(first * shard, last * shard, LANES):
            e = jnp.exp(scores[p, at_row : at_row + LANES, :] - norm)
            probs[at_row : at_row + LANES, lanes_of(p)] = e.astype(jnp.bfloat16)

    sooner = [p for p in (2, 3) if p < pairs]
    later = [p for p in (1, 0) if p < pairs]
    for p in sooner:
        settle(p)
        weigh_again(p, 0, 4)
    for p in later:
        settle(p)
    log_norm = norms[0]
    loss_ref[...] = log_norm - own_score
    own_term = jnp.exp(own_score - log_norm) - 1.0

    d2d_copies, rs_copies = {}, {}

    def exchange(dyl):
        d2d_copies[dyl].wait_recv()
        whole = cgrad[dyl] + d2d_in[dyl].astype(jnp.float32)
        rs[dyl] = whole[rows:].astype(jnp.bfloat16)
        for dyh, dx, dy in far_first:
            if dy == dyl:
                target = grp_at(dyh, dx)
                i = mirror(dyh, dx, dy)
                rs_copies[i] = push(
                    rs.at[dyl, rows_of(pl.multiple_of(target * cut, cut), cut)],
                    rs_in.at[i],
                    rs_sem,
                    i,
                    (target, at(z, dyl, 1)),
                )
        if dyl:
            itm[...] = whole[:rows].astype(jnp.bfloat16)
            return push(itm, itm_in, itm_sem, 0, y_mate)
        cgrad[0, 0:rows, :] = whole[:rows]

    for j in (3, 1, 2, 0):
        for p in later:
            weigh_again(p, j, j + 1)
        grad = jnp.dot(
            probs[j * shard : (j + 1) * shard, :],
            q_all[...],
            preferred_element_type=jnp.float32,
        )
        grad = SCALE * grad
        if j % 2:
            i = j // 2
            d2d[i] = grad.astype(jnp.bfloat16)
            d2d_copies[i] = push(d2d.at[i], d2d_in.at[i], d2d_sem, i, core_mate)
        else:
            cgrad[j // 2] = grad
        if j == 2:
            itm_copy = exchange(1)
    exchange(0)

    own_rows = rows_of(pl.multiple_of(g * cut, cut), cut)
    summed = jnp.zeros((cut, width), jnp.float32)
    for i in range(len(plane)):
        rs_copies[i].wait_recv()
        summed = summed + rs_in[i].astype(jnp.float32)
    red[...] = summed.astype(jnp.bfloat16)
    ag_copies = {}
    for dyh, dx, dyl in far_first:
        if dyl == 0:
            i = mirror(dyh, dx, 0)
            ag_copies[i] = push(
                red, ag.at[own_rows], ag_sem, i, (grp_at(dyh, dx), at(z, 0, 1))
            )

    acc = own_term * cand_t[:, 0:rows].astype(jnp.float32)
    for r in range(nz):
        if r:
            part_copies[r].wait_recv()
            piece = part_in[r]
        else:
            piece = part[pos[0]]
        share = jnp.exp((stats_of(0, r)[0] if r else own["top"]) - log_norm)
        acc = acc + share * piece.astype(jnp.float32)
    qg_ref[...] = (SCALE * acc).T

    itm_copy.wait_recv()
    column = jnp.broadcast_to(own_term, (rows, rows)).T
    column = jnp.concatenate([column] * (width // rows), axis=1)
    vg_ref[...] = (
        cgrad[0, 0:rows, :]
        + itm_in[...].astype(jnp.float32)
        + SCALE * column * q_all[0:rows, :].astype(jnp.float32)
    )

    for i in ag_copies:
        ag_copies[i].wait_recv()
    for copy in started:
        copy.wait_send()


def emit(loss_in, qg_in, vg_in, ng_in, loss, qg, vg, ng, wide, sem):
    copies = [
        pltpu.make_async_copy(qg_in, qg, sem.at[0]),
        pltpu.make_async_copy(vg_in, vg, sem.at[1]),
        pltpu.make_async_copy(loss_in, loss, sem.at[2]),
    ]
    for copy in copies:
        copy.start()
    size = ng_in.shape[0] // 2
    for i in range(2):
        span = pl.ds(i * size, size)
        wide[span, :] = ng_in[span, :].astype(jnp.float32)
        copy = pltpu.make_async_copy(wide.at[span], ng.at[span], sem.at[3 + i])
        copy.start()
        copies.append(copy)
    for copy in copies:
        copy.wait()


def local(queries, items, item_ids, neg_embed, neg_logq, logq_table, *, nz, nx):
    rows, width = queries.shape
    neg_rows = neg_embed.shape[0]
    shard = rows + neg_rows
    tall = 4 * shard
    groups = 2 * nx
    cut = neg_rows // groups
    pairs = nz // 2
    f32, bf16 = jnp.float32, jnp.bfloat16
    dma = pltpu.SemaphoreType.DMA
    vmem = pl.BlockSpec(memory_space=pltpu.VMEM)
    away = pl.BlockSpec(memory_space=pl.ANY)
    table = logq_table.reshape(-1, LANES)
    neg_lines = neg_logq.reshape(-1, LANES)
    results = pl.pallas_call(
        functools.partial(kernel, nz, nx),
        out_shape=(
            pltpu.VMEM((1, rows), f32),
            pltpu.VMEM((rows, width), f32),
            pltpu.VMEM((rows, width), f32),
            pltpu.VMEM((neg_rows, width), bf16),
        ),
        in_specs=[away] * 6,
        out_specs=(vmem, vmem, vmem, vmem),
        scratch_shapes=[
            pltpu.SMEM(item_ids.shape, jnp.int32),
            pltpu.VMEM(table.shape, f32),
            pltpu.VMEM(neg_lines.shape, f32),
            pltpu.VMEM((nz * rows, width), bf16),
            pltpu.VMEM((tall, width), bf16),
            pltpu.VMEM((width, tall), bf16),
            pltpu.VMEM((4, 8, LANES), f32),
            pltpu.VMEM((tall, LANES), f32),
            pltpu.VMEM((rows, LANES), f32),
            pltpu.VMEM((pairs, tall, 2 * rows), f32),
            pltpu.VMEM((tall, nz * rows), bf16),
            pltpu.VMEM((2, shard, width), f32),
            pltpu.VMEM((nz, width, rows), bf16),
            pltpu.VMEM((nz, width, rows), bf16),
            pltpu.VMEM((pairs, 2, 2 * rows), f32),
            pltpu.VMEM((nz, pairs, 2, 2 * rows), f32),
            pltpu.VMEM((2, shard, width), bf16),
            pltpu.VMEM((2, shard, width), bf16),
            pltpu.VMEM((rows, width), bf16),
            pltpu.VMEM((rows, width), bf16),
            pltpu.VMEM((2, neg_rows, width), bf16),
            pltpu.VMEM((2 * groups, cut, width), bf16),
            pltpu.VMEM((cut, width), bf16),
            dma((6,)),
            dma((2, nz + 1)),
            dma((2, 5)),
            dma((2, 4)),
            dma((2, nz * pairs)),
            dma((2, nz)),
            dma((2, 2)),
            dma((2, 1)),
            dma((2, 2 * groups)),
            dma((2, 2 * groups)),
        ],
        compiler_params=pltpu.CompilerParams(
            collective_id=0, has_side_effects=True, vmem_limit_bytes=60 << 20
        ),
    )(queries, items, item_ids, neg_embed, neg_lines, table)
    loss, qg, vg, ng = pl.pallas_call(
        emit,
        out_shape=(
            jax.ShapeDtypeStruct((1, rows), f32),
            jax.ShapeDtypeStruct((rows, width), f32),
            jax.ShapeDtypeStruct((rows, width), f32),
            jax.ShapeDtypeStruct((neg_rows, width), f32),
        ),
        in_specs=[vmem] * 4,
        out_specs=(away, away, away, away),
        scratch_shapes=[pltpu.VMEM((neg_rows, width), f32), dma((5,))],
    )(*(pltpu.with_memory_space_constraint(r, pltpu.VMEM) for r in results))
    return loss.reshape(rows), qg, vg, ng


def solution(mesh):
    return jax.shard_map(
        functools.partial(
            local, nz=mesh.shape["dev"] // 4, nx=mesh.shape["grp"] // 2
        ),
        mesh=mesh,
        in_specs=(
            P(("grp", "dev"), None),
            P(("grp", "dev"), None),
            P("grp"),
            P("dev", None),
            P("dev"),
            P(),
        ),
        out_specs=(
            P(("grp", "dev")),
            P(("grp", "dev"), None),
            P(("grp", "dev"), None),
            P("dev", None),
        ),
        check_vma=False,
    )
```
